512 devices in a mesh: groups: 2 (over y), block: 32 (over z), seg: 4 (over x), sub: 2 (over core).
Axes of the slice: x: 4, y: 2, z: 32, core: 2. Of those that a mesh axis runs over, the one named last changes fastest.
The devices are a block of a 4x8x32 slice.
Arguments:
- old_fields: float32 [32768, 4, 512], P(('groups', 'block', 'seg', 'sub')), parts along dimension 0, may hold values from -6 to 6
- corner_shift: float32 [24, 32768], P(None, ('groups', 'block', 'seg', 'sub')), parts along dimension 1, may hold values from -0.2 to 0.2
- targets: float32 [3, 2097152], P(None, ('groups', 'block', 'seg', 'sub')), parts along dimension 1, may hold values from -0.7 to 0.7
- owners: int32 [16384], P(('groups', 'block', 'seg', 'sub')), parts along dimension 0, may hold values from 0 to 16383, as said below
Outputs:
- new_fields: float32 [4, 2097152], P(None, ('groups', 'block', 'seg', 'sub')), parts along dimension 1
The draws below stay inside these ranges and needn't reach their ends.
There are 2 independent parts, one for each index of `groups`. The reference program is written for one: setup_inputs(seed, part) draws one part's arguments, and reference() takes and returns one part's arrays. A program takes and returns all parts, laid end to end along the dimension named above; each array names one. Nothing has to cross between parts.
Inputs may be any that keep to these rules, and one draw needn't show every extreme that they name: `owners`: owner e lies on device e // 64. At most 2 of the blocks on the rows of one device are owned by elements of any one device, and in every draw some device owns exactly 2 blocks of every device.
All inputs are finite; a program needn't handle non-finite values.
Results may differ from the reference program's by a relative error of at most 0.00029.
Values sent between devices are 32-bit elements; how exact they have to be, the bound alone decides.
No kernel may reach another device: no remote copies, remote signals or barrier semaphores. Data moves between devices by JAX's collectives and lax.ppermute only.
A program may use at most 64 MiB of HBM per device.

```python
import jax
import jax.numpy as jnp
import numpy as np
from jax import lax

NVAR = 4
NODES = 512
NEWTON = 3
CAP = 2
BLK_DEV = 32
E_DEV = 64
ELEMS = 16384
POINTS = 1048576


def draw_owners(key, part):
    device_count = ELEMS // E_DEV
    subkeys = jax.random.split(jax.random.fold_in(key, 7), 4)
    popular = jax.random.randint(subkeys[0], (), 0, device_count)
    others = jax.vmap(lambda sub_key: jax.random.permutation(sub_key, device_count - 1))(jax.random.split(subkeys[1], device_count))
    shuffle = jax.vmap(lambda sub_key: jax.random.permutation(sub_key, BLK_DEV))(jax.random.split(subkeys[2], device_count))
    position = jnp.arange(BLK_DEV, dtype=jnp.int32)
    spread_pick = others[:, (position - CAP) % (device_count - 1)]
    spread_dev = (popular + 1 + spread_pick) % device_count
    owner_dev = jnp.where(position[None, :] < CAP, popular, spread_dev)
    owner_dev = jnp.take_along_axis(owner_dev, shuffle, axis=1)
    element = jax.random.randint(subkeys[3], (device_count, BLK_DEV), 0, E_DEV)
    return (owner_dev * E_DEV + element).reshape(-1).astype(jnp.int32)


def block_scale(stream_key, dims, shards, low, largest):
    def one(axis_at, parts):
        heights = jax.random.uniform(jax.random.fold_in(jax.random.fold_in(stream_key, 6), axis_at), (parts,), jnp.float32, low / len(shards), largest / len(shards))
        return jnp.repeat(jnp.exp(heights), dims[axis_at] // parts).reshape((-1,) + (1,) * (len(dims) - axis_at - 1))

    factor_of = one(*shards[0])
    for cut in shards[1:]:
        factor_of = factor_of * one(*cut)
    return factor_of


def noise(stream_key, dims, scale, limit, cuts=(), held_as=jnp.bfloat16):
    values = jax.random.normal(stream_key, dims, jnp.float32) * scale
    if len(cuts) > 0:
        values = block_scale(stream_key, dims, cuts, -0.22, 0.18) * values
    return jnp.clip(values, min=-limit, max=limit).astype(held_as)


def setup_inputs(seed: int = 0, part: int = 0) -> dict:
    streams_of = jax.random.split(jax.random.key(seed), 5)
    part_splits = jax.random.split(jax.random.fold_in(streams_of[4], part), 5)
    return {
        "old_fields": noise(part_splits[0], (ELEMS, NVAR, NODES), 1.0, 6.0, ((0, 256),), jnp.float32),
        "corner_shift": jnp.clip(jax.random.uniform(part_splits[1], (24, ELEMS), jnp.float32, -0.2, 0.2) * block_scale(part_splits[1], (24, ELEMS), ((1, 256),), -0.4, 0.0), -0.2, 0.2),
        "targets": jnp.clip(jax.random.uniform(part_splits[2], (3, POINTS), jnp.float32, -0.7, 0.7) * block_scale(part_splits[2], (3, POINTS), ((1, 256),), -0.4, 0.0), -0.7, 0.7),
        "owners": draw_owners(jax.random.fold_in(jax.random.fold_in(streams_of[4], part), 71), part),
    }


GLL_POINTS = (-1.0, -0.8717401485096066, -0.5917001814331423, -0.2092992179024789, 0.2092992179024789, 0.5917001814331423, 0.8717401485096066, 1.0)
EXACT = lax.Precision.HIGHEST


def lagrange_rows(coords):
    gll_nodes = jnp.array(GLL_POINTS, jnp.float32)
    offsets = coords[None, :] - gll_nodes[:, None]
    spacing = gll_nodes[:, None] - gll_nodes[None, :] + jnp.eye(8, dtype=jnp.float32)
    diag_mask = jnp.eye(8, dtype=bool)
    factors = jnp.where(diag_mask[:, :, None], 1.0, offsets[None, :, :] / spacing[:, :, None])
    return jnp.prod(factors, axis=1)


def corner_signs():
    bit_table = np.array([[(corner >> (2 - coord_dim)) & 1 for corner in range(8)] for coord_dim in range(3)], np.float32)
    return jnp.asarray(2.0 * bit_table - 1.0)


def outer_prod(first, second, third):
    return (first[:, None, None, :] * second[None, :, None, :] * third[None, None, :, :]).reshape(8, -1)


def trilinear(ref_pos):
    shape_list = []
    slope_list = []
    for coord_dim in range(3):
        coordinate = ref_pos[coord_dim]
        shape_list.append(jnp.stack([0.5 - 0.5 * coordinate, 0.5 + 0.5 * coordinate]))
        slope_list.append(jnp.stack([jnp.full_like(coordinate, -0.5), jnp.full_like(coordinate, 0.5)]))
    values = outer_prod(shape_list[0], shape_list[1], shape_list[2])
    slopes = [outer_prod(slope_list[0], shape_list[1], shape_list[2]),
              outer_prod(shape_list[0], slope_list[1], shape_list[2]),
              outer_prod(shape_list[0], shape_list[1], slope_list[2])]
    return values, slopes


def solve_three(matrix, rhs_rows):
    cofactors = []
    for row_id in range(3):
        keep_rows = [remain for remain in range(3) if remain != row_id]
        cof_row = []
        for col_id in range(3):
            keep_cols = [remain for remain in range(3) if remain != col_id]
            sign_factor = 1.0 if (row_id + col_id) % 2 == 0 else -1.0
            cof_row.append(sign_factor * (matrix[keep_rows[0]][keep_cols[0]] * matrix[keep_rows[1]][keep_cols[1]]
                                          - matrix[keep_rows[0]][keep_cols[1]] * matrix[keep_rows[1]][keep_cols[0]]))
        cofactors.append(cof_row)
    determinant = matrix[0][0] * cofactors[0][0] + matrix[0][1] * cofactors[0][1] + matrix[0][2] * cofactors[0][2]
    return [(cofactors[0][col_id] * rhs_rows[0] + cofactors[1][col_id] * rhs_rows[1] + cofactors[2][col_id] * rhs_rows[2]) / determinant for col_id in range(3)]


def invert_map(corners, target):
    ref_pos = jnp.zeros_like(target)
    for iteration in range(NEWTON):
        values, slopes = trilinear(ref_pos)
        mapped = jnp.dot(corners, values, precision=EXACT)
        columns = [jnp.dot(corners, slope_row, precision=EXACT) for slope_row in slopes]
        matrix = [[columns[col_id][row_id] for col_id in range(3)] for row_id in range(3)]
        misfit = mapped - target
        update = solve_three(matrix, [misfit[row_id] for row_id in range(3)])
        ref_pos = jnp.clip(ref_pos - jnp.stack(update), -1.2, 1.2)
    return ref_pos


def interpolate(element_field, corners, target):
    ref_pos = invert_map(corners, target)
    along_x = lagrange_rows(ref_pos[0])
    along_y = lagrange_rows(ref_pos[1])
    along_z = lagrange_rows(ref_pos[2])
    weights = (along_y[:, None, :] * along_z[None, :, :]).reshape(64, -1)
    var_count = element_field.shape[0]
    partial_sum = jnp.dot(element_field.reshape(var_count * 8, 64), weights, precision=EXACT)
    return jnp.sum(partial_sum.reshape(var_count, 8, -1) * along_x[None, :, :], axis=1)


def reference(old_fields, corner_shift, targets, owners):
    block_count = owners.shape[0]
    block_points = targets.reshape(3, block_count, -1).transpose(1, 0, 2)
    cube_signs = corner_signs()

    def per_block(inputs):
        owner_id, target = inputs
        corners = cube_signs + corner_shift[:, owner_id].reshape(3, 8)
        return interpolate(old_fields[owner_id], corners, target)

    result = lax.map(per_block, (owners, block_points), batch_size=64)
    return result.transpose(1, 0, 2).reshape(old_fields.shape[1], -1)
```

```python
import functools

import jax
import jax.numpy as jnp
import numpy as np
from jax import lax
from jax.experimental import pallas as pl
from jax.experimental.pallas import tpu as pltpu
from jax.sharding import PartitionSpec as P

NEWTON = 3
CAP = 2
FIRST = 7
LANES = 128
ID_LANES = 16
FULLEST, COUNT = ID_LANES - 2, ID_LANES - 1

GLL_POINTS = (
    -1.0,
    -0.8717401485096066,
    -0.5917001814331423,
    -0.2092992179024789,
    0.2092992179024789,
    0.5917001814331423,
    0.8717401485096066,
    1.0,
)
EXACT = lax.Precision.HIGHEST


def monomial_table():
    signs = np.array([[2.0 * (c >> 2 - a & 1) - 1.0 for c in range(8)] for a in range(3)])
    table = np.zeros((24, 24), np.float32)
    offset = np.zeros((24,), np.float32)
    for m in range(8):
        row = np.ones(8)
        for a in range(3):
            if m >> 2 - a & 1:
                row = row * signs[a]
        for a in range(3):
            table[8 * a + m, 8 * a : 8 * a + 8] = row / 8.0
            offset[8 * a + m] = float(np.sum(row * signs[a]) / 8.0)
    return table, offset


def lagrange_constants():
    nodes = np.array(GLL_POINTS, np.float64)
    plain = [0, 1, 2, 3, 4, 5, 6, 7]
    orders = [plain] + [[i] * 4 + [i + 2] * 4 for i in (0, 4, 1, 5)]
    blocks = []
    for order in orders:
        for k in range(7):
            blocks.append([nodes[[m for m in range(8) if m != i][k]] for i in order])
        factor = []
        for i in order:
            others = [nodes[i] - nodes[m] for m in range(8) if m != i]
            factor.append(1.0 / np.prod(others))
        blocks.append(factor)
    table = np.array(blocks, np.float32).reshape(len(orders), 8, 8)
    return np.repeat(table[..., None], LANES, axis=-1)


def pack_kernel(first, slots, row_elems, owners_ref, targets_ref, send_ref, seen, meta):
    rows, last = send_ref.shape[0], 3 * slots
    blocks = targets_ref.shape[0]
    send_ref[...] = jnp.zeros_like(send_ref)
    meta[...] = jnp.zeros_like(meta)
    lane = lax.broadcasted_iota(jnp.int32, (1, LANES), 1)

    def clear(r, carry):
        seen[r] = 0
        return carry

    lax.fori_loop(0, rows, clear, 0)

    def place(b, fullest):
        owner = owners_ref[b]
        r = owner // row_elems
        k = seen[r]
        seen[r] = k + 1

        @pl.when(jnp.logical_and(k >= first, k < first + slots))
        def _():
            slot = k - first
            points = targets_ref[b]
            for a in range(3):
                send_ref[r, pl.ds(slot * 3 + a, 1), :] = points[a : a + 1]
            meta[pl.ds(r, 1), :] += jnp.where(lane == slot, owner - r * row_elems, 0)

        return jnp.maximum(fullest, k + 1)

    fullest = lax.fori_loop(0, blocks, place, jnp.int32(0))

    def count(r, carry):
        used = jnp.clip(seen[r] - first, 0, slots)
        ids = meta[pl.ds(r, 1), :]
        ids = jnp.where(lane == COUNT, used, jnp.where(lane == FULLEST, fullest, ids))
        send_ref[r, pl.ds(last, 1), :] = ids.astype(jnp.float32)
        return carry

    lax.fori_loop(0, rows, count, 0)


def pack(owners, block_points, rows, first, slots, row_elems):
    height = -(-(3 * slots + 1) // 8) * 8
    return pl.pallas_call(
        functools.partial(pack_kernel, first, slots, row_elems),
        out_shape=jax.ShapeDtypeStruct((rows, height, LANES), jnp.float32),
        in_specs=[
            pl.BlockSpec(memory_space=pltpu.SMEM),
            pl.BlockSpec(memory_space=pltpu.VMEM),
        ],
        out_specs=pl.BlockSpec(memory_space=pltpu.VMEM),
        scratch_shapes=[pltpu.SMEM((rows,), jnp.int32), pltpu.VMEM((rows, LANES), jnp.int32)],
        name="pack",
    )(owners, block_points)


def newton(coef, target):
    def mapped(a, m):
        return coef[8 * a + m]

    def solve(jac, misfit):
        cof = [[None] * 3 for _ in range(3)]
        for r in range(3):
            r0, r1 = (r + 1) % 3, (r + 2) % 3
            for c in range(3):
                c0, c1 = (c + 1) % 3, (c + 2) % 3
                cof[r][c] = jac[r0][c0] * jac[r1][c1] - jac[r0][c1] * jac[r1][c0]
        det = jac[0][0] * cof[0][0] + jac[0][1] * cof[0][1] + jac[0][2] * cof[0][2]
        inverse = 1.0 / det
        return [
            (cof[0][c] * misfit[0] + cof[1][c] * misfit[1] + cof[2][c] * misfit[2]) * inverse
            for c in range(3)
        ]

    jac = [[mapped(a, 4), mapped(a, 2), mapped(a, 1)] for a in range(3)]
    step = solve(jac, [mapped(a, 0) - target[a] for a in range(3)])
    pos = [jnp.clip(-s, -1.2, 1.2) for s in step]
    for _ in range(NEWTON - 1):
        u, v, w = pos
        uv, uw, vw = u * v, u * w, v * w
        jac, misfit = [], []
        for a in range(3):
            du = mapped(a, 4) + mapped(a, 6) * v + mapped(a, 5) * w + mapped(a, 7) * vw
            dv = mapped(a, 2) + mapped(a, 6) * u + mapped(a, 3) * w + mapped(a, 7) * uw
            dw = mapped(a, 1) + mapped(a, 5) * u + mapped(a, 3) * v + mapped(a, 7) * uv
            at = mapped(a, 0) + mapped(a, 2) * v + mapped(a, 1) * w + mapped(a, 3) * vw + u * du
            jac.append([du, dv, dw])
            misfit.append(at - target[a])
        step = solve(jac, misfit)
        pos = [jnp.clip(p - s, -1.2, 1.2) for p, s in zip(pos, step)]
    return pos


def lagrange(point, table):
    value = (point - table[0]) * table[7]
    for k in range(1, 7):
        value = value * (point - table[k])
    return value


def halves(value):
    high = value.astype(jnp.bfloat16)
    return high, (value - high.astype(jnp.float32)).astype(jnp.bfloat16)


def evaluate_kernel(elems, meta_ref, recv_ref, const_ref, *refs):
    pieces, (out_ref, table, points, coefs, live, sems) = refs[:8], refs[8:]
    senders = recv_ref.shape[0]
    height = pieces[0].shape[0]
    copies = [
        pltpu.make_async_copy(piece, table.at[pl.ds(k * height, height)], sems.at[k])
        for k, piece in enumerate(pieces)
    ]
    for copy in copies:
        copy.start()

    def of_sender(s, total):
        used = meta_ref[s * ID_LANES + COUNT]

        def of_slot(k, carry):
            live[total + k] = s * ID_LANES + k
            return carry

        lax.fori_loop(0, used, of_slot, 0)
        return total + used

    total = lax.fori_loop(0, senders, of_sender, jnp.int32(0))
    for copy in copies:
        copy.wait()

    lane = lax.broadcasted_iota(jnp.int32, (16, LANES), 1)

    def group(g, carry):
        where = []
        for u in range(8):
            at = live[jnp.minimum(g * 8 + u, total - 1)]
            s, k, code = at // ID_LANES, at % ID_LANES, meta_ref[at]
            base = (code // elems) * height
            elem = code % elems
            where.append((s, k, base + elem * 16))
            for a in range(3):
                points[a, pl.ds(u, 1), :] = recv_ref[s, pl.ds(k * 3 + a, 1), :]
            coefs[pl.ds(u, 1), :] = table[pl.ds(base + elems * 16 + elem, 1), :]
        all_coefs = coefs[...]
        coef = [jnp.broadcast_to(all_coefs[:, m : m + 1], (8, LANES)) for m in range(24)]
        pos = newton(coef, [points[a] for a in range(3)])
        for u in range(8):
            s, k, start = where[u]
            rows = [jnp.broadcast_to(p[u : u + 1], (8, LANES)) for p in pos]
            along_y = lagrange(rows[1], const_ref[0])
            along_z = lagrange(rows[2], const_ref[0])
            weights = jnp.concatenate(
                [jnp.broadcast_to(along_y[j : j + 1], (8, LANES)) * along_z for j in range(8)], axis=0
            )
            weights = jnp.concatenate(halves(weights), axis=0)
            field = table[pl.ds(pl.multiple_of(start, 16), 16), :]
            turned = pltpu.roll(field, LANES // 2, 1)
            even = jnp.where(lane < LANES // 2, field, turned)
            odd = jnp.where(lane < LANES // 2, turned, field)
            both = jnp.concatenate(halves(jnp.concatenate([even, odd], axis=0)), axis=0)
            sums = jnp.dot(both, weights, preferred_element_type=jnp.float32)
            total_x = None
            for q in range(4):
                term = sums[8 * q : 8 * q + 8] + sums[32 + 8 * q : 40 + 8 * q]
                term = term * lagrange(rows[0], const_ref[1 + q])
                total_x = term if total_x is None else total_x + term
            out_ref[s, k] = total_x[0:4] + total_x[4:8]
        return carry

    lax.fori_loop(0, (total + 7) // 8, group, 0)


def evaluate(meta, recv, pieces, slots, elems):
    senders = recv.shape[0]
    height = pieces[0].shape[0]
    constants = lagrange_constants()
    return pl.pallas_call(
        functools.partial(evaluate_kernel, elems),
        out_shape=jax.ShapeDtypeStruct((senders, slots, 4, LANES), jnp.float32),
        in_specs=[pl.BlockSpec(memory_space=pltpu.SMEM)]
        + [pl.BlockSpec(memory_space=pltpu.VMEM)] * 2
        + [pl.BlockSpec(memory_space=pl.ANY)] * 8,
        out_specs=pl.BlockSpec(memory_space=pltpu.VMEM),
        scratch_shapes=[
            pltpu.VMEM((8 * height, LANES), jnp.float32),
            pltpu.VMEM((3, 8, LANES), jnp.float32),
            pltpu.VMEM((8, LANES), jnp.float32),
            pltpu.SMEM((senders * ID_LANES,), jnp.int32),
            pltpu.SemaphoreType.DMA((8,)),
        ],
        name="evaluate",
    )(meta, recv, jnp.asarray(constants), *pieces)


def unpack_kernel(first, slots, row_elems, owners_ref, back_ref, before_ref, out_ref, seen):
    def clear(r, carry):
        seen[r] = 0
        return carry

    lax.fori_loop(0, back_ref.shape[0], clear, 0)

    def take(b, carry):
        r = owners_ref[b] // row_elems
        k = seen[r]
        seen[r] = k + 1
        fits = jnp.logical_and(k >= first, k < first + slots)

        @pl.when(fits)
        def _():
            out_ref[b] = back_ref[r, k - first]

        @pl.when(jnp.logical_not(fits))
        def _():
            out_ref[b] = before_ref[b]

        return carry

    lax.fori_loop(0, out_ref.shape[0], take, 0)


def unpack(owners, back, before, first, slots, row_elems):
    return pl.pallas_call(
        functools.partial(unpack_kernel, first, slots, row_elems),
        out_shape=jax.ShapeDtypeStruct(before.shape, jnp.float32),
        in_specs=[pl.BlockSpec(memory_space=pltpu.SMEM)]
        + [pl.BlockSpec(memory_space=pltpu.VMEM)] * 2,
        out_specs=pl.BlockSpec(memory_space=pltpu.VMEM),
        scratch_shapes=[pltpu.SMEM((back.shape[0],), jnp.int32)],
        name="unpack",
    )(owners, back, before)


def row_pieces(old_fields, corner_shift):
    elems = old_fields.shape[0]
    table, offset = monomial_table()
    coefs = jnp.dot(jnp.asarray(table), corner_shift, precision=EXACT) + offset[:, None]
    coefs = jnp.pad(coefs.T, ((0, 0), (0, LANES - coefs.shape[0])))
    fields = old_fields.reshape(elems, 4, 4, LANES).transpose(0, 2, 1, 3).reshape(-1, LANES)
    own = jnp.concatenate([fields, coefs], axis=0)
    segs = lax.axis_size("seg")

    def along(step):
        return lax.ppermute(own, "seg", [(i, (i + step) % segs) for i in range(segs)])

    half = [own, along(1), along(segs - 1), along(2)]
    return half + [lax.ppermute(piece, "sub", [(0, 1), (1, 0)]) for piece in half]


def all_to_all(array):
    return lax.all_to_all(array, "block", split_axis=0, concat_axis=0, tiled=True)


def shards(old_fields, corner_shift, targets, owners):
    rows = lax.axis_size("block")
    segs, subs = lax.axis_size("seg"), lax.axis_size("sub")
    elems = old_fields.shape[0]
    row_elems = elems * segs * subs
    block_count = owners.shape[0]
    most = CAP * segs * subs
    block_points = targets.reshape(3, block_count, -1).transpose(1, 0, 2)
    pieces = row_pieces(old_fields, corner_shift)

    def trip(first, slots, before):
        recv = all_to_all(pack(owners, block_points, rows, first, slots, row_elems))
        meta = recv[:, 3 * slots, :ID_LANES].astype(jnp.int32)
        device, elem = meta // elems, meta % elems
        apart = (device // subs - lax.axis_index("seg")) % segs
        piece = jnp.where(apart == 0, 0, jnp.where(apart == 1, 2, jnp.where(apart == 2, 3, 1)))
        piece = piece + jnp.where(device % subs == lax.axis_index("sub"), 0, 4)
        is_id = lax.broadcasted_iota(jnp.int32, meta.shape, 1) < FULLEST
        codes = jnp.where(is_id, piece * elems + elem, meta).reshape(-1)
        answers = all_to_all(evaluate(codes, recv, pieces, slots, elems))
        fullest = jnp.max(meta[:, FULLEST])
        return unpack(owners, answers, before, first, slots, row_elems), fullest

    done, fullest = trip(0, FIRST, block_points_like(block_points))
    done = lax.cond(
        fullest > FIRST,
        lambda held: trip(FIRST, most - FIRST, held)[0],
        lambda held: held,
        done,
    )
    return done.transpose(1, 0, 2).reshape(4, -1)


def block_points_like(block_points):
    return jnp.zeros((block_points.shape[0], 4, block_points.shape[2]), jnp.float32)


def solution(mesh):
    split = ("groups", "block", "seg", "sub")
    in_specs = (P(split, None, None), P(None, split), P(None, split), P(split))
    return jax.shard_map(
        shards, mesh=mesh, in_specs=in_specs, out_specs=P(None, split), check_vma=False
    )
```

```python
import functools

import jax
import jax.numpy as jnp
import numpy as np
from jax import lax
from jax.experimental import pallas as pl
from jax.experimental.pallas import tpu as pltpu
from jax.sharding import PartitionSpec as P

NEWTON = 3
CAP = 2
FIRST = 7
LANES = 128
ID_LANES = 16
FULLEST, COUNT = ID_LANES - 2, ID_LANES - 1

GLL_POINTS = (
    -1.0,
    -0.8717401485096066,
    -0.5917001814331423,
    -0.2092992179024789,
    0.2092992179024789,
    0.5917001814331423,
    0.8717401485096066,
    1.0,
)
EXACT = lax.Precision.HIGHEST


def monomial_table():
    signs = np.array([[2.0 * (c >> 2 - a & 1) - 1.0 for c in range(8)] for a in range(3)])
    table = np.zeros((24, 24), np.float32)
    offset = np.zeros((24,), np.float32)
    for m in range(8):
        row = np.ones(8)
        for a in range(3):
            if m >> 2 - a & 1:
                row = row * signs[a]
        for a in range(3):
            table[8 * a + m, 8 * a : 8 * a + 8] = row / 8.0
            offset[8 * a + m] = float(np.sum(row * signs[a]) / 8.0)
    return table, offset


def lagrange_constants():
    nodes = np.array(GLL_POINTS, np.float64)
    plain = [0, 1, 2, 3, 4, 5, 6, 7]
    orders = [plain] + [[i] * 4 + [i + 2] * 4 for i in (0, 4, 1, 5)]
    blocks = []
    for order in orders:
        for k in range(7):
            blocks.append([nodes[[m for m in range(8) if m != i][k]] for i in order])
        factor = []
        for i in order:
            others = [nodes[i] - nodes[m] for m in range(8) if m != i]
            factor.append(1.0 / np.prod(others))
        blocks.append(factor)
    table = np.array(blocks, np.float32).reshape(len(orders), 8, 8)
    return np.repeat(table[..., None], LANES, axis=-1)


def divided(value, by):
    if by & (by - 1) == 0:
        return value >> (by.bit_length() - 1), value & (by - 1)
    return lax.div(value, by), lax.rem(value, by)


def pack_kernel(first, slots, elems, segs, subs, owners, targets, send_ref, at_ref, *scratch):
    owners_ref, targets_ref, seen, meta, sems = scratch
    copies = [
        pltpu.make_async_copy(owners, owners_ref, sems.at[0]),
        pltpu.make_async_copy(targets, targets_ref, sems.at[1]),
    ]
    for copy in copies:
        copy.start()
    rows, last = send_ref.shape[0], 3 * slots
    my_seg, my_sub = lax.axis_index("seg"), lax.axis_index("sub")
    lane = lax.broadcasted_iota(jnp.int32, (1, LANES), 1)
    meta[...] = jnp.zeros_like(meta)
    for r in range(rows):
        seen[r] = 0
    for copy in copies:
        copy.wait()

    def place(b, fullest):
        device, elem = divided(owners_ref[b], elems)
        device, sub = divided(device, subs)
        r, seg = divided(device, segs)
        apart = divided(seg - my_seg + segs, segs)[1]
        code = (apart + jnp.where(sub == my_sub, 0, segs)) * elems + elem
        k = seen[r]
        seen[r] = k + 1
        slot = k - first
        at_ref[b] = jnp.where(jnp.logical_and(slot >= 0, slot < slots), r * slots + slot, -1)

        @pl.when(jnp.logical_and(slot >= 0, slot < slots))
        def _():
            points = targets_ref[b]
            for a in range(3):
                send_ref[r, slot * 3 + a] = points[a : a + 1]
            added = jnp.where(lane == slot, code, jnp.where(lane == COUNT, 1, 0))
            meta[pl.ds(r, 1), :] += added

        return jnp.maximum(fullest, k + 1)

    fullest = lax.fori_loop(0, targets_ref.shape[0], place, jnp.int32(0), unroll=4)
    ids = jnp.where(lane == FULLEST, fullest, meta[...]).astype(jnp.float32)
    for r in range(rows):
        send_ref[r, last] = ids[r : r + 1]


def pack(owners, block_points, rows, first, slots, elems, segs, subs):
    blocks = owners.shape[0]
    return pl.pallas_call(
        functools.partial(pack_kernel, first, slots, elems, segs, subs),
        out_shape=[
            jax.ShapeDtypeStruct((rows, 3 * slots + 1, 1, LANES), jnp.float32),
            jax.ShapeDtypeStruct((blocks,), jnp.int32),
        ],
        in_specs=[pl.BlockSpec(memory_space=pltpu.HBM)] * 2,
        out_specs=[
            pl.BlockSpec(memory_space=pltpu.VMEM),
            pl.BlockSpec(memory_space=pltpu.SMEM),
        ],
        scratch_shapes=[
            pltpu.SMEM(owners.shape, jnp.int32),
            pltpu.VMEM(block_points.shape, jnp.float32),
            pltpu.SMEM((rows,), jnp.int32),
            pltpu.VMEM((rows, LANES), jnp.int32),
            pltpu.SemaphoreType.DMA((2,)),
        ],
        compiler_params=pltpu.CompilerParams(vmem_limit_bytes=4 << 20),
        name="pack",
    )(owners, block_points)


def newton(coef, target):
    def mapped(a, m):
        return coef[8 * a + m]

    def solve(jac, misfit):
        cof = [[None] * 3 for _ in range(3)]
        for r in range(3):
            r0, r1 = (r + 1) % 3, (r + 2) % 3
            for c in range(3):
                c0, c1 = (c + 1) % 3, (c + 2) % 3
                cof[r][c] = jac[r0][c0] * jac[r1][c1] - jac[r0][c1] * jac[r1][c0]
        det = jac[0][0] * cof[0][0] + jac[0][1] * cof[0][1] + jac[0][2] * cof[0][2]
        inverse = 1.0 / det
        return [
            (cof[0][c] * misfit[0] + cof[1][c] * misfit[1] + cof[2][c] * misfit[2]) * inverse
            for c in range(3)
        ]

    jac = [[mapped(a, 4), mapped(a, 2), mapped(a, 1)] for a in range(3)]
    step = solve(jac, [mapped(a, 0) - target[a] for a in range(3)])
    pos = [jnp.clip(-s, -1.2, 1.2) for s in step]
    for _ in range(NEWTON - 1):
        u, v, w = pos
        uv, uw, vw = u * v, u * w, v * w
        jac, misfit = [], []
        for a in range(3):
            du = mapped(a, 4) + mapped(a, 6) * v + mapped(a, 5) * w + mapped(a, 7) * vw
            dv = mapped(a, 2) + mapped(a, 6) * u + mapped(a, 3) * w + mapped(a, 7) * uw
            dw = mapped(a, 1) + mapped(a, 5) * u + mapped(a, 3) * v + mapped(a, 7) * uv
            at = mapped(a, 0) + mapped(a, 2) * v + mapped(a, 1) * w + mapped(a, 3) * vw + u * du
            jac.append([du, dv, dw])
            misfit.append(at - target[a])
        step = solve(jac, misfit)
        pos = [jnp.clip(p - s, -1.2, 1.2) for p, s in zip(pos, step)]
    return pos


def lagrange(point, table):
    value = (point - table[0]) * table[7]
    for k in range(1, 7):
        value = value * (point - table[k])
    return value


def halves(value):
    high = value.astype(jnp.bfloat16)
    return high, (value - high.astype(jnp.float32)).astype(jnp.bfloat16)


def evaluate_kernel(elems, slots, recv_ref, const_ref, *refs):
    pieces, (out_ref, fields, shapes, points, coefs, meta, live, sems) = refs[:8], refs[8:]
    senders = recv_ref.shape[0]
    ids = pltpu.make_async_copy(recv_ref.at[:, 3 * slots, 0, :], meta, sems.at[0])
    ids.start()
    copies = []
    for k, piece in enumerate(pieces):
        size = elems * 16
        copies += [
            pltpu.make_async_copy(
                piece.at[pl.ds(0, size)], fields.at[pl.ds(k * size, size)], sems.at[2 * k + 1]
            ),
            pltpu.make_async_copy(
                piece.at[pl.ds(size, elems)], shapes.at[pl.ds(k * elems, elems)], sems.at[2 * k + 2]
            ),
        ]
    for copy in copies:
        copy.start()
    ids.wait()

    def of_sender(s, total):
        used = meta[s, COUNT].astype(jnp.int32)

        def of_slot(k, carry):
            live[total + k] = s * ID_LANES + k
            return carry

        lax.fori_loop(0, used, of_slot, 0)
        return total + used

    total = lax.fori_loop(0, senders, of_sender, jnp.int32(0))
    for copy in copies:
        copy.wait()

    lane = lax.broadcasted_iota(jnp.int32, (16, LANES), 1)

    def group(g, carry):
        where = []
        for u in range(8):
            s, k = divided(live[jnp.minimum(g * 8 + u, total - 1)], ID_LANES)
            code = meta[s, k].astype(jnp.int32)
            where.append((s * slots + k, code * 16))
            for a in range(3):
                points[a, pl.ds(u, 1), :] = recv_ref[s, k * 3 + a]
            coefs[pl.ds(u, 1), :] = shapes[pl.ds(code, 1), :]
        all_coefs = coefs[...]
        coef = [jnp.broadcast_to(all_coefs[:, m : m + 1], (8, LANES)) for m in range(24)]
        pos = newton(coef, [points[a] for a in range(3)])
        for u in range(8):
            slot, start = where[u]
            rows = [jnp.broadcast_to(p[u : u + 1], (8, LANES)) for p in pos]
            along_y = lagrange(rows[1], const_ref[0])
            along_z = lagrange(rows[2], const_ref[0])
            weights = jnp.concatenate(
                [jnp.broadcast_to(along_y[j : j + 1], (8, LANES)) * along_z for j in range(8)], axis=0
            )
            weights = jnp.concatenate(halves(weights), axis=0)
            field = fields[pl.ds(pl.multiple_of(start, 16), 16), :]
            turned = pltpu.roll(field, LANES // 2, 1)
            even = jnp.where(lane < LANES // 2, field, turned)
            odd = jnp.where(lane < LANES // 2, turned, field)
            both = jnp.concatenate(halves(jnp.concatenate([even, odd], axis=0)), axis=0)
            sums = jnp.dot(both, weights, preferred_element_type=jnp.float32)
            total_x = None
            for q in range(4):
                term = sums[8 * q : 8 * q + 8] + sums[32 + 8 * q : 40 + 8 * q]
                term = term * lagrange(rows[0], const_ref[1 + q])
                total_x = term if total_x is None else total_x + term
            out_ref[slot] = total_x[0:4] + total_x[4:8]
        return carry

    lax.fori_loop(0, (total + 7) // 8, group, 0)


def evaluate(recv, pieces, slots, elems):
    senders = recv.shape[0]
    return pl.pallas_call(
        functools.partial(evaluate_kernel, elems, slots),
        out_shape=jax.ShapeDtypeStruct((senders * slots, 4, LANES), jnp.float32),
        in_specs=[pl.BlockSpec(memory_space=pltpu.VMEM)] * 2
        + [pl.BlockSpec(memory_space=pl.ANY)] * 8,
        out_specs=pl.BlockSpec(memory_space=pltpu.VMEM),
        scratch_shapes=[
            pltpu.VMEM((8 * elems * 16, LANES), jnp.float32),
            pltpu.VMEM((8 * elems, LANES), jnp.float32),
            pltpu.VMEM((3, 8, LANES), jnp.float32),
            pltpu.VMEM((8, LANES), jnp.float32),
            pltpu.SMEM((senders, LANES), jnp.float32),
            pltpu.SMEM((senders * ID_LANES,), jnp.int32),
            pltpu.SemaphoreType.DMA((17,)),
        ],
        compiler_params=pltpu.CompilerParams(vmem_limit_bytes=12 << 20),
        name="evaluate",
    )(recv, jnp.asarray(lagrange_constants()), *pieces)


def unpack_kernel(has_before, at_ref, back_ref, *refs):
    out_ref = refs[-1]
    for b in range(out_ref.shape[0]):
        if has_before:
            at = at_ref[b]
            taken = back_ref[jnp.maximum(at, 0)]
            out_ref[b] = jnp.where(at >= 0, taken, refs[0][b])
        else:
            out_ref[b] = back_ref[jnp.maximum(at_ref[b], 0)]

def unpack(at, back, before):
    held = [] if before is None else [before]
    return pl.pallas_call(
        functools.partial(unpack_kernel, before is not None),
        out_shape=jax.ShapeDtypeStruct((at.shape[0], 4, LANES), jnp.float32),
        in_specs=[pl.BlockSpec(memory_space=pltpu.SMEM)]
        + [pl.BlockSpec(memory_space=pltpu.VMEM)] * (1 + len(held)),
        out_specs=pl.BlockSpec(memory_space=pltpu.VMEM),
        compiler_params=pltpu.CompilerParams(vmem_limit_bytes=4 << 20),
        name="unpack",
    )(at, back, *held)


def row_pieces(old_fields, corner_shift):
    elems = old_fields.shape[0]
    table, offset = monomial_table()
    coefs = jnp.dot(jnp.asarray(table), corner_shift, precision=EXACT) + offset[:, None]
    coefs = jnp.pad(coefs.T, ((0, 0), (0, LANES - coefs.shape[0])))
    fields = old_fields.reshape(elems, 4, 4, LANES).transpose(0, 2, 1, 3).reshape(-1, LANES)
    own = jnp.concatenate([fields, coefs], axis=0)
    segs = lax.axis_size("seg")

    def along(step):
        return lax.ppermute(own, "seg", [(i, (i + step) % segs) for i in range(segs)])

    half = [own] + [along(segs - apart) for apart in range(1, segs)]
    return half + [lax.ppermute(piece, "sub", [(0, 1), (1, 0)]) for piece in half]


def all_to_all(array):
    return lax.all_to_all(array, "block", split_axis=0, concat_axis=0, tiled=True)


def shards(old_fields, corner_shift, targets, owners):
    rows = lax.axis_size("block")
    segs, subs = lax.axis_size("seg"), lax.axis_size("sub")
    elems = old_fields.shape[0]
    most = CAP * segs * subs
    block_points = targets.reshape(3, owners.shape[0], -1).transpose(1, 0, 2)
    pieces = row_pieces(old_fields, corner_shift)

    def trip(first, slots, before):
        send, at = pack(owners, block_points, rows, first, slots, elems, segs, subs)
        recv = all_to_all(send)
        answers = evaluate(recv, pieces, slots, elems).reshape(rows, slots, 4, LANES)
        back = all_to_all(answers).reshape(rows * slots, 4, LANES)
        return unpack(at, back, before), recv[:, 3 * slots, 0, FULLEST]

    done, fullest = trip(0, FIRST, None)
    done = lax.cond(
        jnp.max(fullest) > FIRST,
        lambda held: trip(FIRST, most - FIRST, held)[0],
        lambda held: held,
        done,
    )
    return done.transpose(1, 0, 2).reshape(4, -1)


def solution(mesh):
    split = ("groups", "block", "seg", "sub")
    in_specs = (P(split, None, None), P(None, split), P(None, split), P(split))
    return jax.shard_map(
        shards, mesh=mesh, in_specs=in_specs, out_specs=P(None, split), check_vma=False
    )
```

```python
import functools

import jax
import jax.numpy as jnp
import numpy as np
from jax import lax
from jax.experimental import pallas as pl
from jax.experimental.pallas import tpu as pltpu
from jax.sharding import PartitionSpec as P

NEWTON = 3
CAP = 2
FIRST = 7
LANES = 128
ID_LANES = 16
FULLEST, COUNT = ID_LANES - 2, ID_LANES - 1

GLL_POINTS = (
    -1.0,
    -0.8717401485096066,
    -0.5917001814331423,
    -0.2092992179024789,
    0.2092992179024789,
    0.5917001814331423,
    0.8717401485096066,
    1.0,
)
EXACT = lax.Precision.HIGHEST


def monomial_table():
    signs = np.array([[2.0 * (c >> 2 - a & 1) - 1.0 for c in range(8)] for a in range(3)])
    table = np.zeros((24, 24), np.float32)
    offset = np.zeros((24,), np.float32)
    for m in range(8):
        row = np.ones(8)
        for a in range(3):
            if m >> 2 - a & 1:
                row = row * signs[a]
        for a in range(3):
            table[8 * a + m, 8 * a : 8 * a + 8] = row / 8.0
            offset[8 * a + m] = float(np.sum(row * signs[a]) / 8.0)
    return table, offset


def lagrange_constants():
    nodes = np.array(GLL_POINTS, np.float64)
    others = [[nodes[m] for m in range(8) if m != n] for n in range(8)]
    factor = [1.0 / np.prod([nodes[n] - other for other in others[n]]) for n in range(8)]
    table = np.concatenate([np.array(others).T, np.array(factor)[None]], axis=0)
    return np.repeat(table.astype(np.float32)[..., None], LANES, axis=-1)


def divided(value, by):
    if by & (by - 1) == 0:
        return value >> (by.bit_length() - 1), value & (by - 1)
    return lax.div(value, by), lax.rem(value, by)


def pack_kernel(first, slots, elems, segs, subs, owners, targets, send_ref, at_ref, *scratch):
    owners_ref, targets_ref, seen, meta, sems = scratch
    copies = [
        pltpu.make_async_copy(owners, owners_ref, sems.at[0]),
        pltpu.make_async_copy(targets, targets_ref, sems.at[1]),
    ]
    for copy in copies:
        copy.start()
    rows, last = send_ref.shape[0], 3 * slots
    my_seg, my_sub = lax.axis_index("seg"), lax.axis_index("sub")
    lane = lax.broadcasted_iota(jnp.int32, (1, LANES), 1)
    meta[...] = jnp.zeros_like(meta)
    for r in range(rows):
        seen[r] = 0
    for copy in copies:
        copy.wait()

    def place(b, fullest):
        device, elem = divided(owners_ref[b], elems)
        device, sub = divided(device, subs)
        r, seg = divided(device, segs)
        apart = divided(seg - my_seg + segs, segs)[1]
        code = (apart + jnp.where(sub == my_sub, 0, segs)) * elems + elem
        k = seen[r]
        seen[r] = k + 1
        slot = k - first
        at_ref[b] = jnp.where(jnp.logical_and(slot >= 0, slot < slots), r * slots + slot, -1)

        @pl.when(jnp.logical_and(slot >= 0, slot < slots))
        def _():
            points = targets_ref[b]
            for a in range(3):
                send_ref[r, slot * 3 + a] = points[a : a + 1]
            added = jnp.where(lane == slot, code, jnp.where(lane == COUNT, 1, 0))
            meta[pl.ds(r, 1), :] += added

        return jnp.maximum(fullest, k + 1)

    fullest = lax.fori_loop(0, targets_ref.shape[0], place, jnp.int32(0), unroll=4)
    ids = jnp.where(lane == FULLEST, fullest, meta[...]).astype(jnp.float32)
    for r in range(rows):
        send_ref[r, last] = ids[r : r + 1]


def pack(owners, block_points, rows, first, slots, elems, segs, subs):
    blocks = owners.shape[0]
    return pl.pallas_call(
        functools.partial(pack_kernel, first, slots, elems, segs, subs),
        out_shape=[
            jax.ShapeDtypeStruct((rows, 3 * slots + 1, 1, LANES), jnp.float32),
            jax.ShapeDtypeStruct((blocks,), jnp.int32),
        ],
        in_specs=[pl.BlockSpec(memory_space=pltpu.HBM)] * 2,
        out_specs=[
            pl.BlockSpec(memory_space=pltpu.VMEM),
            pl.BlockSpec(memory_space=pltpu.SMEM),
        ],
        scratch_shapes=[
            pltpu.SMEM(owners.shape, jnp.int32),
            pltpu.VMEM(block_points.shape, jnp.float32),
            pltpu.SMEM((rows,), jnp.int32),
            pltpu.VMEM((rows, LANES), jnp.int32),
            pltpu.SemaphoreType.DMA((2,)),
        ],
        compiler_params=pltpu.CompilerParams(vmem_limit_bytes=4 << 20),
        name="pack",
    )(owners, block_points)


def newton(coef, target):
    def mapped(a, m):
        return coef[8 * a + m]

    def solve(jac, misfit):
        cof = [[None] * 3 for _ in range(3)]
        for r in range(3):
            r0, r1 = (r + 1) % 3, (r + 2) % 3
            for c in range(3):
                c0, c1 = (c + 1) % 3, (c + 2) % 3
                cof[r][c] = jac[r0][c0] * jac[r1][c1] - jac[r0][c1] * jac[r1][c0]
        det = jac[0][0] * cof[0][0] + jac[0][1] * cof[0][1] + jac[0][2] * cof[0][2]
        inverse = 1.0 / det
        return [
            (cof[0][c] * misfit[0] + cof[1][c] * misfit[1] + cof[2][c] * misfit[2]) * inverse
            for c in range(3)
        ]

    jac = [[mapped(a, 4), mapped(a, 2), mapped(a, 1)] for a in range(3)]
    step = solve(jac, [mapped(a, 0) - target[a] for a in range(3)])
    pos = [jnp.clip(-s, -1.2, 1.2) for s in step]
    for _ in range(NEWTON - 1):
        u, v, w = pos
        uv, uw, vw = u * v, u * w, v * w
        jac, misfit = [], []
        for a in range(3):
            du = mapped(a, 4) + mapped(a, 6) * v + mapped(a, 5) * w + mapped(a, 7) * vw
            dv = mapped(a, 2) + mapped(a, 6) * u + mapped(a, 3) * w + mapped(a, 7) * uw
            dw = mapped(a, 1) + mapped(a, 5) * u + mapped(a, 3) * v + mapped(a, 7) * uv
            at = mapped(a, 0) + mapped(a, 2) * v + mapped(a, 1) * w + mapped(a, 3) * vw + u * du
            jac.append([du, dv, dw])
            misfit.append(at - target[a])
        step = solve(jac, misfit)
        pos = [jnp.clip(p - s, -1.2, 1.2) for p, s in zip(pos, step)]
    return pos


def lagrange(point, table):
    value = (point - table[0]) * table[7]
    for k in range(1, 7):
        value = value * (point - table[k])
    return value


def halves(value):
    high = value.astype(jnp.bfloat16)
    return high, (value - high.astype(jnp.float32)).astype(jnp.bfloat16)


def segments(elems, lengths):
    size, found, piece, row = elems * 16, [], 0, 0
    for index, length in enumerate(lengths):
        here = 0
        while here < length:
            end = size if row < size else size + elems
            count = min(length - here, end - row)
            base = piece * size + row if row < size else piece * elems + row - size
            found.append((index, here, count, row >= size, base))
            here, row = here + count, row + count
            if row == size + elems:
                piece, row = piece + 1, 0
    return found


def evaluate_kernel(elems, slots, arrays, recv_ref, const_ref, *refs):
    pieces, (out_ref, fields, shapes, points, coefs, meta, live, sems) = refs[:arrays], refs[arrays:]
    senders = recv_ref.shape[0]
    ids = pltpu.make_async_copy(recv_ref.at[:, 3 * slots, 0, :], meta, sems.at[0])
    ids.start()
    copies = []
    for n, (index, row, count, of_coefs, there) in enumerate(
        segments(elems, [piece.shape[0] for piece in pieces])
    ):
        target = (shapes if of_coefs else fields).at[pl.ds(there, count)]
        source = pieces[index].at[pl.ds(row, count)]
        copies.append(pltpu.make_async_copy(source, target, sems.at[n + 1]))
    for copy in copies:
        copy.start()
    ids.wait()

    def of_sender(s, total):
        used = meta[s, COUNT].astype(jnp.int32)

        def of_slot(k, carry):
            live[total + k] = s * ID_LANES + k
            return carry

        lax.fori_loop(0, used, of_slot, 0)
        return total + used

    total = lax.fori_loop(0, senders, of_sender, jnp.int32(0))
    for copy in copies:
        copy.wait()

    lane = lax.broadcasted_iota(jnp.int32, (16, LANES), 1)
    upper = lax.broadcasted_iota(jnp.int32, (8, LANES), 0) < 4

    def gather(g):
        where = []
        for u in range(8):
            s, k = divided(live[jnp.clip(g * 8 + u, 0, jnp.maximum(total - 1, 0))], ID_LANES)
            code = meta[s, k].astype(jnp.int32)
            where += [s * slots + k, code * 16]
            for a in range(3):
                points[a, pl.ds(u, 1), :] = recv_ref[s, k * 3 + a]
            coefs[pl.ds(u, 1), :] = shapes[pl.ds(code, 1), :]
        return tuple(where) + (points[0], points[1], points[2], coefs[...])

    def group(g, held):
        where, target, all_coefs = held[:16], held[16:19], held[19]
        following = gather(g + 1)
        coef = [jnp.broadcast_to(all_coefs[:, m : m + 1], (8, LANES)) for m in range(24)]
        pos = newton(coef, target)
        for u in range(8):
            slot, start = where[2 * u : 2 * u + 2]
            along_x, along_y, along_z = [
                lagrange(jnp.broadcast_to(p[u : u + 1], (8, LANES)), const_ref) for p in pos
            ]
            weights = jnp.concatenate(
                [jnp.broadcast_to(along_y[j : j + 1], (8, LANES)) * along_z for j in range(8)], axis=0
            )
            weights = jnp.concatenate(halves(weights), axis=0)
            field = fields[pl.ds(pl.multiple_of(start, 16), 16), :]
            turned = pltpu.roll(field, LANES // 2, 1)
            even = jnp.where(lane < LANES // 2, field, turned)
            odd = jnp.where(lane < LANES // 2, turned, field)
            both = jnp.concatenate(halves(jnp.concatenate([even, odd], axis=0)), axis=0)
            sums = jnp.dot(both, weights, preferred_element_type=jnp.float32)
            total_x = None
            for q, i in enumerate((0, 4, 1, 5)):
                term = sums[8 * q : 8 * q + 8] + sums[32 + 8 * q : 40 + 8 * q]
                rows = [jnp.broadcast_to(along_x[r : r + 1], (8, LANES)) for r in (i, i + 2)]
                term = term * jnp.where(upper, rows[0], rows[1])
                total_x = term if total_x is None else total_x + term
            out_ref[slot] = total_x[0:4] + total_x[4:8]
        return following

    @pl.when(total > 0)
    def _():
        lax.fori_loop(0, (total + 7) // 8, group, gather(jnp.int32(0)))


def evaluate(recv, pieces, slots, elems):
    senders = recv.shape[0]
    return pl.pallas_call(
        functools.partial(evaluate_kernel, elems, slots, len(pieces)),
        out_shape=jax.ShapeDtypeStruct((senders * slots, 4, LANES), jnp.float32),
        in_specs=[pl.BlockSpec(memory_space=pltpu.VMEM)] * 2
        + [pl.BlockSpec(memory_space=pl.ANY)] * len(pieces),
        out_specs=pl.BlockSpec(memory_space=pltpu.VMEM),
        scratch_shapes=[
            pltpu.VMEM((8 * elems * 16, LANES), jnp.float32),
            pltpu.VMEM((8 * elems, LANES), jnp.float32),
            pltpu.VMEM((3, 8, LANES), jnp.float32),
            pltpu.VMEM((8, LANES), jnp.float32),
            pltpu.SMEM((senders, LANES), jnp.float32),
            pltpu.SMEM((senders * ID_LANES,), jnp.int32),
            pltpu.SemaphoreType.DMA((1 + len(segments(elems, [p.shape[0] for p in pieces])),)),
        ],
        compiler_params=pltpu.CompilerParams(vmem_limit_bytes=12 << 20),
        name="evaluate",
    )(recv, jnp.asarray(lagrange_constants()), *pieces)


def unpack_kernel(has_before, at_ref, back_ref, *refs):
    out_ref = refs[-1]
    for b in range(out_ref.shape[0]):
        if has_before:
            at = at_ref[b]
            taken = back_ref[jnp.maximum(at, 0)]
            out_ref[b] = jnp.where(at >= 0, taken, refs[0][b])
        else:
            out_ref[b] = back_ref[jnp.maximum(at_ref[b], 0)]

def unpack(at, back, before):
    held = [] if before is None else [before]
    return pl.pallas_call(
        functools.partial(unpack_kernel, before is not None),
        out_shape=jax.ShapeDtypeStruct((at.shape[0], 4, LANES), jnp.float32),
        in_specs=[pl.BlockSpec(memory_space=pltpu.SMEM)]
        + [pl.BlockSpec(memory_space=pltpu.VMEM)] * (1 + len(held)),
        out_specs=pl.BlockSpec(memory_space=pltpu.VMEM),
        compiler_params=pltpu.CompilerParams(vmem_limit_bytes=4 << 20),
        name="unpack",
    )(at, back, *held)


def row_pieces(old_fields, corner_shift):
    elems = old_fields.shape[0]
    table, offset = monomial_table()
    coefs = jnp.dot(jnp.asarray(table), corner_shift, precision=EXACT) + offset[:, None]
    coefs = jnp.pad(coefs.T, ((0, 0), (0, LANES - coefs.shape[0])))
    fields = old_fields.reshape(elems, 4, 4, LANES).transpose(0, 2, 1, 3).reshape(-1, LANES)
    own = jnp.concatenate([fields, coefs], axis=0)
    segs = lax.axis_size("seg")
    middle = own.shape[0] // 16 * 8

    def along(array, step):
        return lax.ppermute(array, "seg", [(i, (i + step) % segs) for i in range(segs)])

    before = along(own, 1)
    after = along(own, segs - 1)
    opposite = [along(own[:middle], 2), along(before[middle:], 1)]
    half = [own, after, *opposite, before]
    return half + [lax.ppermute(piece, "sub", [(0, 1), (1, 0)]) for piece in half]


def all_to_all(array):
    return lax.all_to_all(array, "block", split_axis=0, concat_axis=0, tiled=True)


def shards(old_fields, corner_shift, targets, owners):
    rows = lax.axis_size("block")
    segs, subs = lax.axis_size("seg"), lax.axis_size("sub")
    elems = old_fields.shape[0]
    most = CAP * segs * subs
    block_points = targets.reshape(3, owners.shape[0], -1).transpose(1, 0, 2)
    pieces = row_pieces(old_fields, corner_shift)

    def trip(first, slots, before):
        send, at = pack(owners, block_points, rows, first, slots, elems, segs, subs)
        recv = all_to_all(send)
        answers = evaluate(recv, pieces, slots, elems).reshape(rows, slots, 4, LANES)
        back = all_to_all(answers).reshape(rows * slots, 4, LANES)
        return unpack(at, back, before), recv[:, 3 * slots, 0, FULLEST]

    done, fullest = trip(0, FIRST, None)
    done = lax.cond(
        jnp.max(fullest) > FIRST,
        lambda held: trip(FIRST, most - FIRST, held)[0],
        lambda held: held,
        done,
    )
    return done.transpose(1, 0, 2).reshape(4, -1)


def solution(mesh):
    split = ("groups", "block", "seg", "sub")
    in_specs = (P(split, None, None), P(None, split), P(None, split), P(split))
    return jax.shard_map(
        shards, mesh=mesh, in_specs=in_specs, out_specs=P(None, split), check_vma=False
    )
```

```python
import functools

import jax
import jax.numpy as jnp
import numpy as np
from jax import lax
from jax.experimental import pallas as pl
from jax.experimental.pallas import tpu as pltpu
from jax.sharding import PartitionSpec as P

NEWTON = 3
CAP = 2
FIRST = 7
LANES = 128
ID_LANES = 16
FULLEST, COUNT = ID_LANES - 2, ID_LANES - 1

GLL_POINTS = (
    -1.0,
    -0.8717401485096066,
    -0.5917001814331423,
    -0.2092992179024789,
    0.2092992179024789,
    0.5917001814331423,
    0.8717401485096066,
    1.0,
)
EXACT = lax.Precision.HIGHEST


def monomial_table():
    signs = np.array([[2.0 * (c >> 2 - a & 1) - 1.0 for c in range(8)] for a in range(3)])
    table = np.zeros((24, 24), np.float32)
    offset = np.zeros((24,), np.float32)
    for m in range(8):
        row = np.ones(8)
        for a in range(3):
            if m >> 2 - a & 1:
                row = row * signs[a]
        for a in range(3):
            table[8 * a + m, 8 * a : 8 * a + 8] = row / 8.0
            offset[8 * a + m] = float(np.sum(row * signs[a]) / 8.0)
    return table, offset


def lagrange_constants():
    nodes = np.array(GLL_POINTS, np.float64)
    others = [[nodes[m] for m in range(8) if m != n] for n in range(8)]
    factor = [1.0 / np.prod([nodes[n] - other for other in others[n]]) for n in range(8)]
    table = np.concatenate([np.array(others).T, np.array(factor)[None]], axis=0)
    return np.repeat(table.astype(np.float32)[..., None], LANES, axis=-1)


def divided(value, by):
    if by & (by - 1) == 0:
        return value >> (by.bit_length() - 1), value & (by - 1)
    return lax.div(value, by), lax.rem(value, by)


def pack_kernel(first, slots, elems, segs, subs, owners, targets, send_ref, at_ref, *scratch):
    owners_ref, targets_ref, seen, meta, sems = scratch
    copies = [
        pltpu.make_async_copy(owners, owners_ref, sems.at[0]),
        pltpu.make_async_copy(targets, targets_ref, sems.at[1]),
    ]
    for copy in copies:
        copy.start()
    rows, last = send_ref.shape[0], 3 * slots
    my_seg, my_sub = lax.axis_index("seg"), lax.axis_index("sub")
    lane = lax.broadcasted_iota(jnp.int32, (1, LANES), 1)
    meta[...] = jnp.zeros_like(meta)
    for r in range(rows):
        seen[r] = 0
    for copy in copies:
        copy.wait()

    def place(b, fullest):
        device, elem = divided(owners_ref[b], elems)
        device, sub = divided(device, subs)
        r, seg = divided(device, segs)
        apart = divided(seg - my_seg + segs, segs)[1]
        code = (apart + jnp.where(sub == my_sub, 0, segs)) * elems + elem
        k = seen[r]
        seen[r] = k + 1
        slot = k - first
        at_ref[b] = jnp.where(jnp.logical_and(slot >= 0, slot < slots), r * slots + slot, -1)

        @pl.when(jnp.logical_and(slot >= 0, slot < slots))
        def _():
            points = targets_ref[b]
            for a in range(3):
                send_ref[r, slot * 3 + a] = points[a : a + 1]
            added = jnp.where(lane == slot, code, jnp.where(lane == COUNT, 1, 0))
            meta[pl.ds(r, 1), :] += added

        return jnp.maximum(fullest, k + 1)

    fullest = lax.fori_loop(0, targets_ref.shape[0], place, jnp.int32(0), unroll=4)
    ids = jnp.where(lane == FULLEST, fullest, meta[...]).astype(jnp.float32)
    for r in range(rows):
        send_ref[r, last] = ids[r : r + 1]


def pack(owners, block_points, rows, first, slots, elems, segs, subs):
    blocks = owners.shape[0]
    return pl.pallas_call(
        functools.partial(pack_kernel, first, slots, elems, segs, subs),
        out_shape=[
            jax.ShapeDtypeStruct((rows, 3 * slots + 1, 1, LANES), jnp.float32),
            jax.ShapeDtypeStruct((blocks,), jnp.int32),
        ],
        in_specs=[pl.BlockSpec(memory_space=pltpu.HBM)] * 2,
        out_specs=[
            pl.BlockSpec(memory_space=pltpu.VMEM),
            pl.BlockSpec(memory_space=pltpu.SMEM),
        ],
        scratch_shapes=[
            pltpu.SMEM(owners.shape, jnp.int32),
            pltpu.VMEM(block_points.shape, jnp.float32),
            pltpu.SMEM((rows,), jnp.int32),
            pltpu.VMEM((rows, LANES), jnp.int32),
            pltpu.SemaphoreType.DMA((2,)),
        ],
        compiler_params=pltpu.CompilerParams(vmem_limit_bytes=4 << 20),
        name="pack",
    )(owners, block_points)


def newton(coef, target):
    def mapped(a, m):
        return coef[8 * a + m]

    def solve(jac, misfit):
        cof = [[None] * 3 for _ in range(3)]
        for r in range(3):
            r0, r1 = (r + 1) % 3, (r + 2) % 3
            for c in range(3):
                c0, c1 = (c + 1) % 3, (c + 2) % 3
                cof[r][c] = jac[r0][c0] * jac[r1][c1] - jac[r0][c1] * jac[r1][c0]
        det = jac[0][0] * cof[0][0] + jac[0][1] * cof[0][1] + jac[0][2] * cof[0][2]
        inverse = 1.0 / det
        return [
            (cof[0][c] * misfit[0] + cof[1][c] * misfit[1] + cof[2][c] * misfit[2]) * inverse
            for c in range(3)
        ]

    jac = [[mapped(a, 4), mapped(a, 2), mapped(a, 1)] for a in range(3)]
    step = solve(jac, [mapped(a, 0) - target[a] for a in range(3)])
    pos = [jnp.clip(-s, -1.2, 1.2) for s in step]
    for _ in range(NEWTON - 1):
        u, v, w = pos
        uv, uw, vw = u * v, u * w, v * w
        jac, misfit = [], []
        for a in range(3):
            du = mapped(a, 4) + mapped(a, 6) * v + mapped(a, 5) * w + mapped(a, 7) * vw
            dv = mapped(a, 2) + mapped(a, 6) * u + mapped(a, 3) * w + mapped(a, 7) * uw
            dw = mapped(a, 1) + mapped(a, 5) * u + mapped(a, 3) * v + mapped(a, 7) * uv
            at = mapped(a, 0) + mapped(a, 2) * v + mapped(a, 1) * w + mapped(a, 3) * vw + u * du
            jac.append([du, dv, dw])
            misfit.append(at - target[a])
        step = solve(jac, misfit)
        pos = [jnp.clip(p - s, -1.2, 1.2) for p, s in zip(pos, step)]
    return pos


def lagrange(point, table):
    value = (point - table[0]) * table[7]
    for k in range(1, 7):
        value = value * (point - table[k])
    return value


def halves(value):
    high = value.astype(jnp.bfloat16)
    return high, (value - high.astype(jnp.float32)).astype(jnp.bfloat16)


def segments(elems, lengths):
    size, found, piece, row = elems * 16, [], 0, 0
    for index, length in enumerate(lengths):
        here = 0
        while here < length:
            end = size if row < size else size + elems
            count = min(length - here, end - row)
            base = piece * size + row if row < size else piece * elems + row - size
            found.append((index, here, count, row >= size, base))
            here, row = here + count, row + count
            if row == size + elems:
                piece, row = piece + 1, 0
    return found


def evaluate_kernel(elems, slots, arrays, recv_ref, const_ref, *refs):
    pieces, (out_ref, fields, shapes, points, coefs, meta, live, sems) = refs[:arrays], refs[arrays:]
    senders = recv_ref.shape[0]
    ids = pltpu.make_async_copy(recv_ref.at[:, 3 * slots, 0, :], meta, sems.at[0])
    ids.start()
    copies = []
    for n, (index, row, count, of_coefs, there) in enumerate(
        segments(elems, [piece.shape[0] for piece in pieces])
    ):
        target = (shapes if of_coefs else fields).at[pl.ds(there, count)]
        source = pieces[index].at[pl.ds(row, count)]
        copies.append(pltpu.make_async_copy(source, target, sems.at[n + 1]))
    for copy in copies:
        copy.start()
    ids.wait()

    def of_sender(s, total):
        used = meta[s, COUNT].astype(jnp.int32)

        def of_slot(k, carry):
            live[total + k] = s * ID_LANES + k
            return carry

        lax.fori_loop(0, used, of_slot, 0)
        return total + used

    total = lax.fori_loop(0, senders, of_sender, jnp.int32(0))
    for copy in copies:
        copy.wait()

    lane = lax.broadcasted_iota(jnp.int32, (16, LANES), 1)
    upper = lax.broadcasted_iota(jnp.int32, (8, LANES), 0) < 4

    def gather(g):
        where = []
        for u in range(8):
            s, k = divided(live[jnp.clip(g * 8 + u, 0, jnp.maximum(total - 1, 0))], ID_LANES)
            code = meta[s, k].astype(jnp.int32)
            where += [s * slots + k, code * 16]
            for a in range(3):
                points[a, pl.ds(u, 1), :] = recv_ref[s, k * 3 + a]
            coefs[pl.ds(u, 1), :] = shapes[pl.ds(code, 1), :]
        return tuple(where) + (points[0], points[1], points[2], coefs[...])

    def group(g, held):
        where, target, all_coefs = held[:16], held[16:19], held[19]
        following = gather(g + 1)
        coef = [jnp.broadcast_to(all_coefs[:, m : m + 1], (8, LANES)) for m in range(24)]
        pos = newton(coef, target)
        for u in range(8):
            slot, start = where[2 * u : 2 * u + 2]
            along_x, along_y, along_z = [
                lagrange(jnp.broadcast_to(p[u : u + 1], (8, LANES)), const_ref) for p in pos
            ]
            weights = jnp.concatenate(
                [jnp.broadcast_to(along_y[j : j + 1], (8, LANES)) * along_z for j in range(8)], axis=0
            )
            weights = jnp.concatenate(halves(weights), axis=0)
            field = fields[pl.ds(pl.multiple_of(start, 16), 16), :]
            turned = pltpu.roll(field, LANES // 2, 1)
            even = jnp.where(lane < LANES // 2, field, turned)
            odd = jnp.where(lane < LANES // 2, turned, field)
            both = jnp.concatenate(halves(jnp.concatenate([even, odd], axis=0)), axis=0)
            sums = jnp.dot(both, weights, preferred_element_type=jnp.float32)
            total_x = None
            for q, i in enumerate((0, 4, 1, 5)):
                term = sums[8 * q : 8 * q + 8] + sums[32 + 8 * q : 40 + 8 * q]
                rows = [jnp.broadcast_to(along_x[r : r + 1], (8, LANES)) for r in (i, i + 2)]
                term = term * jnp.where(upper, rows[0], rows[1])
                total_x = term if total_x is None else total_x + term
            out_ref[slot] = total_x[0:4] + total_x[4:8]
        return following

    @pl.when(total > 0)
    def _():
        lax.fori_loop(0, (total + 7) // 8, group, gather(jnp.int32(0)))


def evaluate(recv, pieces, slots, elems):
    senders = recv.shape[0]
    return pl.pallas_call(
        functools.partial(evaluate_kernel, elems, slots, len(pieces)),
        out_shape=jax.ShapeDtypeStruct((senders * slots, 4, LANES), jnp.float32),
        in_specs=[pl.BlockSpec(memory_space=pltpu.VMEM)] * 2
        + [pl.BlockSpec(memory_space=pl.ANY)] * len(pieces),
        out_specs=pl.BlockSpec(memory_space=pltpu.VMEM),
        scratch_shapes=[
            pltpu.VMEM((8 * elems * 16, LANES), jnp.float32),
            pltpu.VMEM((8 * elems, LANES), jnp.float32),
            pltpu.VMEM((3, 8, LANES), jnp.float32),
            pltpu.VMEM((8, LANES), jnp.float32),
            pltpu.SMEM((senders, LANES), jnp.float32),
            pltpu.SMEM((senders * ID_LANES,), jnp.int32),
            pltpu.SemaphoreType.DMA((1 + len(segments(elems, [p.shape[0] for p in pieces])),)),
        ],
        compiler_params=pltpu.CompilerParams(vmem_limit_bytes=12 << 20),
        name="evaluate",
    )(recv, jnp.asarray(lagrange_constants()), *pieces)


def unpack_kernel(has_before, at_ref, back_ref, *refs):
    out_ref = refs[-1]
    for b in range(out_ref.shape[0]):
        if has_before:
            at = at_ref[b]
            taken = back_ref[jnp.maximum(at, 0)]
            out_ref[b] = jnp.where(at >= 0, taken, refs[0][b])
        else:
            out_ref[b] = back_ref[jnp.maximum(at_ref[b], 0)]

def unpack(at, back, before):
    held = [] if before is None else [before]
    return pl.pallas_call(
        functools.partial(unpack_kernel, before is not None),
        out_shape=jax.ShapeDtypeStruct((at.shape[0], 4, LANES), jnp.float32),
        in_specs=[pl.BlockSpec(memory_space=pltpu.SMEM)]
        + [pl.BlockSpec(memory_space=pltpu.VMEM)] * (1 + len(held)),
        out_specs=pl.BlockSpec(memory_space=pltpu.VMEM),
        compiler_params=pltpu.CompilerParams(vmem_limit_bytes=4 << 20),
        name="unpack",
    )(at, back, *held)


def row_pieces(old_fields, corner_shift):
    elems = old_fields.shape[0]
    table, offset = monomial_table()
    coefs = jnp.dot(jnp.asarray(table), corner_shift, precision=EXACT) + offset[:, None]
    coefs = jnp.pad(coefs.T, ((0, 0), (0, LANES - coefs.shape[0])))
    fields = old_fields.reshape(elems, 4, 4, LANES).transpose(0, 2, 1, 3).reshape(-1, LANES)
    own = jnp.concatenate([fields, coefs], axis=0)
    segs = lax.axis_size("seg")
    middle = own.shape[0] // 16 * 8

    def along(array, step):
        return lax.ppermute(array, "seg", [(i, (i + step) % segs) for i in range(segs)])

    before = along(own, 1)
    after = along(own, segs - 1)
    opposite = [along(after[:middle], segs - 1), along(before[middle:], 1)]
    half = [own, after, *opposite, before]
    return half + [lax.ppermute(piece, "sub", [(0, 1), (1, 0)]) for piece in half]


def all_to_all(array):
    return lax.all_to_all(array, "block", split_axis=0, concat_axis=0, tiled=True)


def shards(old_fields, corner_shift, targets, owners):
    rows = lax.axis_size("block")
    segs, subs = lax.axis_size("seg"), lax.axis_size("sub")
    elems = old_fields.shape[0]
    most = CAP * segs * subs
    block_points = targets.reshape(3, owners.shape[0], -1).transpose(1, 0, 2)
    pieces = row_pieces(old_fields, corner_shift)

    def trip(first, slots, before):
        send, at = pack(owners, block_points, rows, first, slots, elems, segs, subs)
        recv = all_to_all(send)
        answers = evaluate(recv, pieces, slots, elems).reshape(rows, slots, 4, LANES)
        back = all_to_all(answers).reshape(rows * slots, 4, LANES)
        return unpack(at, back, before), recv[:, 3 * slots, 0, FULLEST]

    done, fullest = trip(0, FIRST, None)
    done = lax.cond(
        jnp.max(fullest) > FIRST,
        lambda held: trip(FIRST, most - FIRST, held)[0],
        lambda held: held,
        done,
    )
    return done.transpose(1, 0, 2).reshape(4, -1)


def solution(mesh):
    split = ("groups", "block", "seg", "sub")
    in_specs = (P(split, None, None), P(None, split), P(None, split), P(split))
    return jax.shard_map(
        shards, mesh=mesh, in_specs=in_specs, out_specs=P(None, split), check_vma=False
    )
```

```python
import functools

import jax
import jax.numpy as jnp
import numpy as np
from jax import lax
from jax.experimental import pallas as pl
from jax.experimental.pallas import tpu as pltpu
from jax.sharding import PartitionSpec as P

NEWTON = 3
CAP = 2
FIRST = 7
LANES = 128
ID_LANES = 16
FULLEST, COUNT = ID_LANES - 2, ID_LANES - 1

GLL_POINTS = (
    -1.0,
    -0.8717401485096066,
    -0.5917001814331423,
    -0.2092992179024789,
    0.2092992179024789,
    0.5917001814331423,
    0.8717401485096066,
    1.0,
)
EXACT = lax.Precision.HIGHEST


def monomial_table():
    signs = np.array([[2.0 * (c >> 2 - a & 1) - 1.0 for c in range(8)] for a in range(3)])
    table = np.zeros((24, 24), np.float32)
    offset = np.zeros((24,), np.float32)
    for m in range(8):
        row = np.ones(8)
        for a in range(3):
            if m >> 2 - a & 1:
                row = row * signs[a]
        for a in range(3):
            table[8 * a + m, 8 * a : 8 * a + 8] = row / 8.0
            offset[8 * a + m] = float(np.sum(row * signs[a]) / 8.0)
    return table, offset


def lagrange_constants():
    nodes = np.array(GLL_POINTS, np.float64)
    others = [[nodes[m] for m in range(8) if m != n] for n in range(8)]
    factor = [1.0 / np.prod([nodes[n] - other for other in others[n]]) for n in range(8)]
    table = np.concatenate([np.array(others).T, np.array(factor)[None]], axis=0)
    return np.repeat(table.astype(np.float32)[..., None], LANES, axis=-1)


def divided(value, by):
    if by & (by - 1) == 0:
        return value >> (by.bit_length() - 1), value & (by - 1)
    return lax.div(value, by), lax.rem(value, by)


def pack_kernel(first, slots, elems, segs, subs, owners, targets, send_ref, at_ref, *scratch):
    owners_ref, targets_ref, seen, meta, sems = scratch
    copies = [
        pltpu.make_async_copy(owners, owners_ref, sems.at[0]),
        pltpu.make_async_copy(targets, targets_ref, sems.at[1]),
    ]
    for copy in copies:
        copy.start()
    rows, last = send_ref.shape[0], 3 * slots
    my_seg, my_sub = lax.axis_index("seg"), lax.axis_index("sub")
    lane = lax.broadcasted_iota(jnp.int32, (1, LANES), 1)
    meta[...] = jnp.zeros_like(meta)
    for r in range(rows):
        seen[r] = 0
    for copy in copies:
        copy.wait()

    def place(b, fullest):
        device, elem = divided(owners_ref[b], elems)
        device, sub = divided(device, subs)
        r, seg = divided(device, segs)
        apart = divided(seg - my_seg + segs, segs)[1]
        code = (apart + jnp.where(sub == my_sub, 0, segs)) * elems + elem
        k = seen[r]
        seen[r] = k + 1
        slot = k - first
        at_ref[b] = jnp.where(jnp.logical_and(slot >= 0, slot < slots), r * slots + slot, -1)

        @pl.when(jnp.logical_and(slot >= 0, slot < slots))
        def _():
            points = targets_ref[b]
            for a in range(3):
                send_ref[r, slot * 3 + a] = points[a : a + 1]
            added = jnp.where(lane == slot, code, jnp.where(lane == COUNT, 1, 0))
            meta[pl.ds(r, 1), :] += added

        return jnp.maximum(fullest, k + 1)

    fullest = lax.fori_loop(0, targets_ref.shape[0], place, jnp.int32(0), unroll=4)
    ids = jnp.where(lane == FULLEST, fullest, meta[...]).astype(jnp.float32)
    for r in range(rows):
        send_ref[r, last] = ids[r : r + 1]


def pack(owners, block_points, rows, first, slots, elems, segs, subs):
    blocks = owners.shape[0]
    return pl.pallas_call(
        functools.partial(pack_kernel, first, slots, elems, segs, subs),
        out_shape=[
            jax.ShapeDtypeStruct((rows, 3 * slots + 1, 1, LANES), jnp.float32),
            jax.ShapeDtypeStruct((blocks,), jnp.int32),
        ],
        in_specs=[pl.BlockSpec(memory_space=pltpu.HBM)] * 2,
        out_specs=[
            pl.BlockSpec(memory_space=pltpu.VMEM),
            pl.BlockSpec(memory_space=pltpu.SMEM),
        ],
        scratch_shapes=[
            pltpu.SMEM(owners.shape, jnp.int32),
            pltpu.VMEM(block_points.shape, jnp.float32),
            pltpu.SMEM((rows,), jnp.int32),
            pltpu.VMEM((rows, LANES), jnp.int32),
            pltpu.SemaphoreType.DMA((2,)),
        ],
        compiler_params=pltpu.CompilerParams(vmem_limit_bytes=4 << 20),
        name="pack",
    )(owners, block_points)


def newton(coef, target):
    def mapped(a, m):
        return coef[8 * a + m]

    def solve(jac, misfit):
        cof = [[None] * 3 for _ in range(3)]
        for r in range(3):
            r0, r1 = (r + 1) % 3, (r + 2) % 3
            for c in range(3):
                c0, c1 = (c + 1) % 3, (c + 2) % 3
                cof[r][c] = jac[r0][c0] * jac[r1][c1] - jac[r0][c1] * jac[r1][c0]
        det = jac[0][0] * cof[0][0] + jac[0][1] * cof[0][1] + jac[0][2] * cof[0][2]
        inverse = 1.0 / det
        return [
            (cof[0][c] * misfit[0] + cof[1][c] * misfit[1] + cof[2][c] * misfit[2]) * inverse
            for c in range(3)
        ]

    jac = [[mapped(a, 4), mapped(a, 2), mapped(a, 1)] for a in range(3)]
    step = solve(jac, [mapped(a, 0) - target[a] for a in range(3)])
    pos = [jnp.clip(-s, -1.2, 1.2) for s in step]
    for _ in range(NEWTON - 1):
        u, v, w = pos
        uv, uw, vw = u * v, u * w, v * w
        jac, misfit = [], []
        for a in range(3):
            du = mapped(a, 4) + mapped(a, 6) * v + mapped(a, 5) * w + mapped(a, 7) * vw
            dv = mapped(a, 2) + mapped(a, 6) * u + mapped(a, 3) * w + mapped(a, 7) * uw
            dw = mapped(a, 1) + mapped(a, 5) * u + mapped(a, 3) * v + mapped(a, 7) * uv
            at = mapped(a, 0) + mapped(a, 2) * v + mapped(a, 1) * w + mapped(a, 3) * vw + u * du
            jac.append([du, dv, dw])
            misfit.append(at - target[a])
        step = solve(jac, misfit)
        pos = [jnp.clip(p - s, -1.2, 1.2) for p, s in zip(pos, step)]
    return pos


def lagrange(point, table):
    value = (point - table[0]) * table[7]
    for k in range(1, 7):
        value = value * (point - table[k])
    return value


def halves(value):
    high = value.astype(jnp.bfloat16)
    return high, (value - high.astype(jnp.float32)).astype(jnp.bfloat16)


def segments(elems, lengths):
    size, found, piece, row = elems * 16, [], 0, 0
    for index, length in enumerate(lengths):
        here = 0
        while here < length:
            end = size if row < size else size + elems
            count = min(length - here, end - row)
            base = piece * size + row if row < size else piece * elems + row - size
            found.append((index, here, count, row >= size, base))
            here, row = here + count, row + count
            if row == size + elems:
                piece, row = piece + 1, 0
    return found


def evaluate_kernel(elems, slots, arrays, recv_ref, const_ref, *refs):
    pieces, (out_ref, fields, shapes, points, coefs, meta, live, sems) = refs[:arrays], refs[arrays:]
    senders = recv_ref.shape[0]
    ids = pltpu.make_async_copy(recv_ref.at[:, 3 * slots, 0, :], meta, sems.at[0])
    ids.start()
    copies = []
    for n, (index, row, count, of_coefs, there) in enumerate(
        segments(elems, [piece.shape[0] for piece in pieces])
    ):
        target = (shapes if of_coefs else fields).at[pl.ds(there, count)]
        source = pieces[index].at[pl.ds(row, count)]
        copies.append(pltpu.make_async_copy(source, target, sems.at[n + 1]))
    for copy in copies:
        copy.start()
    ids.wait()

    def of_sender(s, total):
        used = meta[s, COUNT].astype(jnp.int32)

        def of_slot(k, carry):
            live[total + k] = s * ID_LANES + k
            return carry

        lax.fori_loop(0, used, of_slot, 0)
        return total + used

    total = lax.fori_loop(0, senders, of_sender, jnp.int32(0))
    for copy in copies:
        copy.wait()

    lane = lax.broadcasted_iota(jnp.int32, (16, LANES), 1)
    upper = lax.broadcasted_iota(jnp.int32, (8, LANES), 0) < 4

    def gather(g):
        where = []
        for u in range(8):
            s, k = divided(live[jnp.clip(g * 8 + u, 0, jnp.maximum(total - 1, 0))], ID_LANES)
            code = meta[s, k].astype(jnp.int32)
            where += [s * slots + k, code * 16]
            for a in range(3):
                points[a, pl.ds(u, 1), :] = recv_ref[s, k * 3 + a]
            coefs[pl.ds(u, 1), :] = shapes[pl.ds(code, 1), :]
        return tuple(where) + (points[0], points[1], points[2], coefs[...])

    def group(g, held):
        where, target, all_coefs = held[:16], held[16:19], held[19]
        following = gather(g + 1)
        coef = [jnp.broadcast_to(all_coefs[:, m : m + 1], (8, LANES)) for m in range(24)]
        pos = newton(coef, target)
        for u in range(8):
            slot, start = where[2 * u : 2 * u + 2]
            along_x, along_y, along_z = [
                lagrange(jnp.broadcast_to(p[u : u + 1], (8, LANES)), const_ref) for p in pos
            ]
            weights = jnp.concatenate(
                [jnp.broadcast_to(along_y[j : j + 1], (8, LANES)) * along_z for j in range(8)], axis=0
            )
            weights = jnp.concatenate(halves(weights), axis=0)
            field = fields[pl.ds(pl.multiple_of(start, 16), 16), :]
            turned = pltpu.roll(field, LANES // 2, 1)
            even = jnp.where(lane < LANES // 2, field, turned)
            odd = jnp.where(lane < LANES // 2, turned, field)
            both = jnp.concatenate(halves(jnp.concatenate([even, odd], axis=0)), axis=0)
            sums = jnp.dot(both, weights, preferred_element_type=jnp.float32)
            total_x = None
            for q, i in enumerate((0, 4, 1, 5)):
                term = sums[8 * q : 8 * q + 8] + sums[32 + 8 * q : 40 + 8 * q]
                rows = [jnp.broadcast_to(along_x[r : r + 1], (8, LANES)) for r in (i, i + 2)]
                term = term * jnp.where(upper, rows[0], rows[1])
                total_x = term if total_x is None else total_x + term
            out_ref[slot] = total_x[0:4] + total_x[4:8]
        return following

    @pl.when(total > 0)
    def _():
        lax.fori_loop(0, (total + 7) // 8, group, gather(jnp.int32(0)))


def evaluate(recv, pieces, slots, elems):
    senders = recv.shape[0]
    return pl.pallas_call(
        functools.partial(evaluate_kernel, elems, slots, len(pieces)),
        out_shape=jax.ShapeDtypeStruct((senders * slots, 4, LANES), jnp.float32),
        in_specs=[pl.BlockSpec(memory_space=pltpu.VMEM)] * 2
        + [pl.BlockSpec(memory_space=pl.ANY)] * len(pieces),
        out_specs=pl.BlockSpec(memory_space=pltpu.VMEM),
        scratch_shapes=[
            pltpu.VMEM((8 * elems * 16, LANES), jnp.float32),
            pltpu.VMEM((8 * elems, LANES), jnp.float32),
            pltpu.VMEM((3, 8, LANES), jnp.float32),
            pltpu.VMEM((8, LANES), jnp.float32),
            pltpu.SMEM((senders, LANES), jnp.float32),
            pltpu.SMEM((senders * ID_LANES,), jnp.int32),
            pltpu.SemaphoreType.DMA((1 + len(segments(elems, [p.shape[0] for p in pieces])),)),
        ],
        compiler_params=pltpu.CompilerParams(vmem_limit_bytes=12 << 20),
        name="evaluate",
    )(recv, jnp.asarray(lagrange_constants()), *pieces)


def unpack_kernel(has_before, at_ref, back_ref, *refs):
    out_ref = refs[-1]
    for b in range(out_ref.shape[0]):
        if has_before:
            at = at_ref[b]
            taken = back_ref[jnp.maximum(at, 0)]
            out_ref[b] = jnp.where(at >= 0, taken, refs[0][b])
        else:
            out_ref[b] = back_ref[jnp.maximum(at_ref[b], 0)]

def unpack(at, back, before):
    held = [] if before is None else [before]
    return pl.pallas_call(
        functools.partial(unpack_kernel, before is not None),
        out_shape=jax.ShapeDtypeStruct((at.shape[0], 4, LANES), jnp.float32),
        in_specs=[pl.BlockSpec(memory_space=pltpu.SMEM)]
        + [pl.BlockSpec(memory_space=pltpu.VMEM)] * (1 + len(held)),
        out_specs=pl.BlockSpec(memory_space=pltpu.VMEM),
        compiler_params=pltpu.CompilerParams(vmem_limit_bytes=4 << 20),
        name="unpack",
    )(at, back, *held)


def row_pieces(old_fields, corner_shift):
    elems = old_fields.shape[0]
    table, offset = monomial_table()
    coefs = jnp.dot(jnp.asarray(table), corner_shift, precision=EXACT) + offset[:, None]
    coefs = jnp.pad(coefs.T, ((0, 0), (0, LANES - coefs.shape[0])))
    fields = old_fields.reshape(elems, 4, 4, LANES).transpose(0, 2, 1, 3).reshape(-1, LANES)
    own = jnp.concatenate([fields, coefs], axis=0)
    segs = lax.axis_size("seg")
    middle = own.shape[0] * 2 // 40 * 8

    def along(array, step):
        return lax.ppermute(array, "seg", [(i, (i + step) % segs) for i in range(segs)])

    def swapped(array):
        return lax.ppermute(array, "sub", [(0, 1), (1, 0)])

    before = along(own, 1)
    after = along(own, segs - 1)
    near = along(own[:middle], 2)
    far = along(before[middle:], 1)
    opposite = jnp.concatenate([near, far], axis=0)
    half = [own, after, opposite, before]
    return half + [swapped(piece) for piece in half]


def all_to_all(array):
    return lax.all_to_all(array, "block", split_axis=0, concat_axis=0, tiled=True)


def shards(old_fields, corner_shift, targets, owners):
    rows = lax.axis_size("block")
    segs, subs = lax.axis_size("seg"), lax.axis_size("sub")
    elems = old_fields.shape[0]
    most = CAP * segs * subs
    block_points = targets.reshape(3, owners.shape[0], -1).transpose(1, 0, 2)
    pieces = row_pieces(old_fields, corner_shift)

    def trip(first, slots, before):
        send, at = pack(owners, block_points, rows, first, slots, elems, segs, subs)
        recv = all_to_all(send)
        answers = evaluate(recv, pieces, slots, elems).reshape(rows, slots, 4, LANES)
        back = all_to_all(answers).reshape(rows * slots, 4, LANES)
        return unpack(at, back, before), recv[:, 3 * slots, 0, FULLEST]

    done, fullest = trip(0, FIRST, None)
    done = lax.cond(
        jnp.max(fullest) > FIRST,
        lambda held: trip(FIRST, most - FIRST, held)[0],
        lambda held: held,
        done,
    )
    return done.transpose(1, 0, 2).reshape(4, -1)


def solution(mesh):
    split = ("groups", "block", "seg", "sub")
    in_specs = (P(split, None, None), P(None, split), P(None, split), P(split))
    return jax.shard_map(
        shards, mesh=mesh, in_specs=in_specs, out_specs=P(None, split), check_vma=False
    )
```

```python
import functools

import jax
import jax.numpy as jnp
import numpy as np
from jax import lax
from jax.experimental import pallas as pl
from jax.experimental.pallas import tpu as pltpu
from jax.sharding import PartitionSpec as P


NEWTON = 3
CAP = 2
FIRST = 7
LANES = 128
ID_LANES = 16
FULLEST, COUNT = ID_LANES - 2, ID_LANES - 1

GLL_POINTS = (
    -1.0,
    -0.8717401485096066,
    -0.5917001814331423,
    -0.2092992179024789,
    0.2092992179024789,
    0.5917001814331423,
    0.8717401485096066,
    1.0,
)
EXACT = lax.Precision.HIGHEST


def monomial_table():
    signs = np.array([[2.0 * (c >> 2 - a & 1) - 1.0 for c in range(8)] for a in range(3)])
    table = np.zeros((24, 24), np.float32)
    offset = np.zeros((24,), np.float32)
    for m in range(8):
        row = np.ones(8)
        for a in range(3):
            if m >> 2 - a & 1:
                row = row * signs[a]
        for a in range(3):
            table[8 * a + m, 8 * a : 8 * a + 8] = row / 8.0
            offset[8 * a + m] = float(np.sum(row * signs[a]) / 8.0)
    return table, offset


def lagrange_constants():
    nodes = np.array(GLL_POINTS, np.float64)
    others = [[nodes[m] for m in range(8) if m != n] for n in range(8)]
    factor = [1.0 / np.prod([nodes[n] - other for other in others[n]]) for n in range(8)]
    table = np.concatenate([np.array(others).T, np.array(factor)[None]], axis=0)
    return np.repeat(table.astype(np.float32)[..., None], LANES, axis=-1)


def divided(value, by):
    if by & (by - 1) == 0:
        return value >> (by.bit_length() - 1), value & (by - 1)
    return lax.div(value, by), lax.rem(value, by)


def pack_kernel(first, slots, elems, segs, subs, owners, targets, send_ref, at_ref, *scratch):
    owners_ref, targets_ref, seen, meta, sems = scratch
    copies = [
        pltpu.make_async_copy(owners, owners_ref, sems.at[0]),
        pltpu.make_async_copy(targets, targets_ref, sems.at[1]),
    ]
    for copy in copies:
        copy.start()
    rows, last = send_ref.shape[0], 3 * slots
    my_seg, my_sub = lax.axis_index("seg"), lax.axis_index("sub")
    lane = lax.broadcasted_iota(jnp.int32, (1, LANES), 1)
    meta[...] = jnp.zeros_like(meta)
    for r in range(rows):
        seen[r] = 0
    for copy in copies:
        copy.wait()

    def place(b, fullest):
        device, elem = divided(owners_ref[b], elems)
        device, sub = divided(device, subs)
        r, seg = divided(device, segs)
        apart = divided(seg - my_seg + segs, segs)[1]
        code = (apart + jnp.where(sub == my_sub, 0, segs)) * elems + elem
        k = seen[r]
        seen[r] = k + 1
        slot = k - first
        at_ref[b] = jnp.where(jnp.logical_and(slot >= 0, slot < slots), r * slots + slot, -1)

        @pl.when(jnp.logical_and(slot >= 0, slot < slots))
        def _():
            points = targets_ref[b]
            for a in range(3):
                send_ref[r, slot * 3 + a] = points[a : a + 1]
            added = jnp.where(lane == slot, code, jnp.where(lane == COUNT, 1, 0))
            meta[pl.ds(r, 1), :] += added

        return jnp.maximum(fullest, k + 1)

    fullest = lax.fori_loop(0, targets_ref.shape[0], place, jnp.int32(0), unroll=4)
    ids = jnp.where(lane == FULLEST, fullest, meta[...]).astype(jnp.float32)
    for r in range(rows):
        send_ref[r, last] = ids[r : r + 1]


def pack(owners, block_points, rows, first, slots, elems, segs, subs):
    blocks = owners.shape[0]
    return pl.pallas_call(
        functools.partial(pack_kernel, first, slots, elems, segs, subs),
        out_shape=[
            jax.ShapeDtypeStruct((rows, 3 * slots + 1, 1, LANES), jnp.float32),
            jax.ShapeDtypeStruct((blocks,), jnp.int32),
        ],
        in_specs=[pl.BlockSpec(memory_space=pltpu.HBM)] * 2,
        out_specs=[
            pl.BlockSpec(memory_space=pltpu.VMEM),
            pl.BlockSpec(memory_space=pltpu.SMEM),
        ],
        scratch_shapes=[
            pltpu.SMEM(owners.shape, jnp.int32),
            pltpu.VMEM(block_points.shape, jnp.float32),
            pltpu.SMEM((rows,), jnp.int32),
            pltpu.VMEM((rows, LANES), jnp.int32),
            pltpu.SemaphoreType.DMA((2,)),
        ],
        compiler_params=pltpu.CompilerParams(vmem_limit_bytes=4 << 20),
        name="pack",
    )(owners, block_points)


def newton(coef, target):
    def mapped(a, m):
        return coef[8 * a + m]

    def solve(jac, misfit):
        cof = [[None] * 3 for _ in range(3)]
        for r in range(3):
            r0, r1 = (r + 1) % 3, (r + 2) % 3
            for c in range(3):
                c0, c1 = (c + 1) % 3, (c + 2) % 3
                cof[r][c] = jac[r0][c0] * jac[r1][c1] - jac[r0][c1] * jac[r1][c0]
        det = jac[0][0] * cof[0][0] + jac[0][1] * cof[0][1] + jac[0][2] * cof[0][2]
        inverse = 1.0 / det
        return [
            (cof[0][c] * misfit[0] + cof[1][c] * misfit[1] + cof[2][c] * misfit[2]) * inverse
            for c in range(3)
        ]

    jac = [[mapped(a, 4), mapped(a, 2), mapped(a, 1)] for a in range(3)]
    step = solve(jac, [mapped(a, 0) - target[a] for a in range(3)])
    pos = [jnp.clip(-s, -1.2, 1.2) for s in step]
    for _ in range(NEWTON - 1):
        u, v, w = pos
        uv, uw, vw = u * v, u * w, v * w
        jac, misfit = [], []
        for a in range(3):
            du = mapped(a, 4) + mapped(a, 6) * v + mapped(a, 5) * w + mapped(a, 7) * vw
            dv = mapped(a, 2) + mapped(a, 6) * u + mapped(a, 3) * w + mapped(a, 7) * uw
            dw = mapped(a, 1) + mapped(a, 5) * u + mapped(a, 3) * v + mapped(a, 7) * uv
            at = mapped(a, 0) + mapped(a, 2) * v + mapped(a, 1) * w + mapped(a, 3) * vw + u * du
            jac.append([du, dv, dw])
            misfit.append(at - target[a])
        step = solve(jac, misfit)
        pos = [jnp.clip(p - s, -1.2, 1.2) for p, s in zip(pos, step)]
    return pos


def lagrange(point, table):
    value = (point - table[0]) * table[7]
    for k in range(1, 7):
        value = value * (point - table[k])
    return value


def halves(value):
    high = value.astype(jnp.bfloat16)
    return high, (value - high.astype(jnp.float32)).astype(jnp.bfloat16)


def segments(elems, lengths):
    size, found, piece, row = elems * 16, [], 0, 0
    for index, length in enumerate(lengths):
        here = 0
        while here < length:
            end = size if row < size else size + elems
            count = min(length - here, end - row)
            base = piece * size + row if row < size else piece * elems + row - size
            found.append((index, here, count, row >= size, base))
            here, row = here + count, row + count
            if row == size + elems:
                piece, row = piece + 1, 0
    return found


def evaluate_kernel(elems, slots, arrays, recv_ref, const_ref, *refs):
    pieces, (out_ref, fields, shapes, points, coefs, meta, live, sems) = refs[:arrays], refs[arrays:]
    senders = recv_ref.shape[0]
    ids = pltpu.make_async_copy(recv_ref.at[:, 3 * slots, 0, :], meta, sems.at[0])
    ids.start()
    copies = []
    for n, (index, row, count, of_coefs, there) in enumerate(
        segments(elems, [piece.shape[0] for piece in pieces])
    ):
        target = (shapes if of_coefs else fields).at[pl.ds(there, count)]
        source = pieces[index].at[pl.ds(row, count)]
        copies.append(pltpu.make_async_copy(source, target, sems.at[n + 1]))
    for copy in copies:
        copy.start()
    ids.wait()

    def of_sender(s, total):
        used = meta[s, COUNT].astype(jnp.int32)

        def of_slot(k, carry):
            live[total + k] = s * ID_LANES + k
            return carry

        lax.fori_loop(0, used, of_slot, 0)
        return total + used

    total = lax.fori_loop(0, senders, of_sender, jnp.int32(0))
    for copy in copies:
        copy.wait()

    lane = lax.broadcasted_iota(jnp.int32, (16, LANES), 1)
    upper = lax.broadcasted_iota(jnp.int32, (8, LANES), 0) < 4

    def gather(g):
        where = []
        for u in range(8):
            s, k = divided(live[jnp.clip(g * 8 + u, 0, jnp.maximum(total - 1, 0))], ID_LANES)
            code = meta[s, k].astype(jnp.int32)
            where += [s * slots + k, code * 16]
            for a in range(3):
                points[a, pl.ds(u, 1), :] = recv_ref[s, k * 3 + a]
            coefs[pl.ds(u, 1), :] = shapes[pl.ds(code, 1), :]
        return tuple(where) + (points[0], points[1], points[2], coefs[...])

    def group(g, held):
        where, target, all_coefs = held[:16], held[16:19], held[19]
        following = gather(g + 1)
        coef = [jnp.broadcast_to(all_coefs[:, m : m + 1], (8, LANES)) for m in range(24)]
        pos = newton(coef, target)
        for u in range(8):
            slot, start = where[2 * u : 2 * u + 2]
            along_x, along_y, along_z = [
                lagrange(jnp.broadcast_to(p[u : u + 1], (8, LANES)), const_ref) for p in pos
            ]
            weights = jnp.concatenate(
                [jnp.broadcast_to(along_y[j : j + 1], (8, LANES)) * along_z for j in range(8)], axis=0
            )
            weights = jnp.concatenate(halves(weights), axis=0)
            field = fields[pl.ds(pl.multiple_of(start, 16), 16), :]
            turned = pltpu.roll(field, LANES // 2, 1)
            even = jnp.where(lane < LANES // 2, field, turned)
            odd = jnp.where(lane < LANES // 2, turned, field)
            both = jnp.concatenate(halves(jnp.concatenate([even, odd], axis=0)), axis=0)
            sums = jnp.dot(both, weights, preferred_element_type=jnp.float32)
            total_x = None
            for q, i in enumerate((0, 4, 1, 5)):
                term = sums[8 * q : 8 * q + 8] + sums[32 + 8 * q : 40 + 8 * q]
                rows = [jnp.broadcast_to(along_x[r : r + 1], (8, LANES)) for r in (i, i + 2)]
                term = term * jnp.where(upper, rows[0], rows[1])
                total_x = term if total_x is None else total_x + term
            out_ref[slot] = total_x[0:4] + total_x[4:8]
        return following

    @pl.when(total > 0)
    def _():
        lax.fori_loop(0, (total + 7) // 8, group, gather(jnp.int32(0)))


def evaluate(recv, pieces, slots, elems):
    senders = recv.shape[0]
    return pl.pallas_call(
        functools.partial(evaluate_kernel, elems, slots, len(pieces)),
        out_shape=jax.ShapeDtypeStruct((senders * slots, 4, LANES), jnp.float32),
        in_specs=[pl.BlockSpec(memory_space=pltpu.VMEM)] * 2
        + [pl.BlockSpec(memory_space=pl.ANY)] * len(pieces),
        out_specs=pl.BlockSpec(memory_space=pltpu.VMEM),
        scratch_shapes=[
            pltpu.VMEM((8 * elems * 16, LANES), jnp.float32),
            pltpu.VMEM((8 * elems, LANES), jnp.float32),
            pltpu.VMEM((3, 8, LANES), jnp.float32),
            pltpu.VMEM((8, LANES), jnp.float32),
            pltpu.SMEM((senders, LANES), jnp.float32),
            pltpu.SMEM((senders * ID_LANES,), jnp.int32),
            pltpu.SemaphoreType.DMA((1 + len(segments(elems, [p.shape[0] for p in pieces])),)),
        ],
        compiler_params=pltpu.CompilerParams(vmem_limit_bytes=12 << 20),
        name="evaluate",
    )(recv, jnp.asarray(lagrange_constants()), *pieces)


def unpack_kernel(has_before, at_ref, back_ref, *refs):
    out_ref = refs[-1]
    for b in range(out_ref.shape[0]):
        if has_before:
            at = at_ref[b]
            taken = back_ref[jnp.maximum(at, 0)]
            out_ref[b] = jnp.where(at >= 0, taken, refs[0][b])
        else:
            out_ref[b] = back_ref[jnp.maximum(at_ref[b], 0)]


def unpack(at, back, before):
    held = [] if before is None else [before]
    return pl.pallas_call(
        functools.partial(unpack_kernel, before is not None),
        out_shape=jax.ShapeDtypeStruct((at.shape[0], 4, LANES), jnp.float32),
        in_specs=[pl.BlockSpec(memory_space=pltpu.SMEM)]
        + [pl.BlockSpec(memory_space=pltpu.VMEM)] * (1 + len(held)),
        out_specs=pl.BlockSpec(memory_space=pltpu.VMEM),
        compiler_params=pltpu.CompilerParams(vmem_limit_bytes=4 << 20),
        name="unpack",
    )(at, back, *held)


def row_pieces(old_fields, corner_shift):
    elems = old_fields.shape[0]
    table, offset = monomial_table()
    coefs = jnp.dot(jnp.asarray(table), corner_shift, precision=EXACT) + offset[:, None]
    coefs = jnp.pad(coefs.T, ((0, 0), (0, LANES - coefs.shape[0])))
    fields = old_fields.reshape(elems, 4, 4, LANES).transpose(0, 2, 1, 3).reshape(-1, LANES)
    own = jnp.concatenate([fields, coefs], axis=0)
    segs = lax.axis_size("seg")
    middle = own.shape[0] * 9 // 160 * 8

    def along(array, step):
        return lax.ppermute(array, "seg", [(i, (i + step) % segs) for i in range(segs)])

    def swapped(array):
        return lax.ppermute(array, "sub", [(0, 1), (1, 0)])

    before = along(own, 1)
    after = along(own, segs - 1)
    near = along(own[:middle], 2)
    far = along(before[middle:], 1)
    opposite = [jnp.concatenate([near, far], axis=0)]
    swaps = [swapped(own), swapped(after)]
    swaps += [swapped(opposite[0]), swapped(before)]
    return [own, after, *opposite, before, *swaps]


def all_to_all(array):
    return lax.all_to_all(array, "block", split_axis=0, concat_axis=0, tiled=True)


def shards(old_fields, corner_shift, targets, owners):
    rows = lax.axis_size("block")
    segs, subs = lax.axis_size("seg"), lax.axis_size("sub")
    elems = old_fields.shape[0]
    most = CAP * segs * subs
    block_points = targets.reshape(3, owners.shape[0], -1).transpose(1, 0, 2)
    pieces = row_pieces(old_fields, corner_shift)

    def trip(first, slots, before):
        send, at = pack(owners, block_points, rows, first, slots, elems, segs, subs)
        recv = all_to_all(send)
        answers = evaluate(recv, pieces, slots, elems).reshape(rows, slots, 4, LANES)
        back = all_to_all(answers).reshape(rows * slots, 4, LANES)
        return unpack(at, back, before), recv[:, 3 * slots, 0, FULLEST]

    done, fullest = trip(0, FIRST, None)
    done = lax.cond(
        jnp.max(fullest) > FIRST,
        lambda held: trip(FIRST, most - FIRST, held)[0],
        lambda held: held,
        done,
    )
    return done.transpose(1, 0, 2).reshape(4, -1)


def solution(mesh):
    split = ("groups", "block", "seg", "sub")
    in_specs = (P(split, None, None), P(None, split), P(None, split), P(split))
    return jax.shard_map(
        shards, mesh=mesh, in_specs=in_specs, out_specs=P(None, split), check_vma=False
    )
```

```python
import functools

import jax
import jax.numpy as jnp
import numpy as np
from jax import lax
from jax.experimental import pallas as pl
from jax.experimental.pallas import tpu as pltpu
from jax.sharding import PartitionSpec as P


NEWTON = 3
CAP = 2
FIRST = 7
LANES = 128
ID_LANES = 16
FULLEST, COUNT = ID_LANES - 2, ID_LANES - 1

GLL_POINTS = (
    -1.0,
    -0.8717401485096066,
    -0.5917001814331423,
    -0.2092992179024789,
    0.2092992179024789,
    0.5917001814331423,
    0.8717401485096066,
    1.0,
)
EXACT = lax.Precision.HIGHEST


def monomial_table():
    signs = np.array([[2.0 * (c >> 2 - a & 1) - 1.0 for c in range(8)] for a in range(3)])
    table = np.zeros((24, 24), np.float32)
    offset = np.zeros((24,), np.float32)
    for m in range(8):
        row = np.ones(8)
        for a in range(3):
            if m >> 2 - a & 1:
                row = row * signs[a]
        for a in range(3):
            table[8 * a + m, 8 * a : 8 * a + 8] = row / 8.0
            offset[8 * a + m] = float(np.sum(row * signs[a]) / 8.0)
    return table, offset


def lagrange_constants():
    nodes = np.array(GLL_POINTS, np.float64)
    others = [[nodes[m] for m in range(8) if m != n] for n in range(8)]
    factor = [1.0 / np.prod([nodes[n] - other for other in others[n]]) for n in range(8)]
    table = np.concatenate([np.array(others).T, np.array(factor)[None]], axis=0)
    return np.repeat(table.astype(np.float32)[..., None], LANES, axis=-1)


def divided(value, by):
    if by & (by - 1) == 0:
        return value >> (by.bit_length() - 1), value & (by - 1)
    return lax.div(value, by), lax.rem(value, by)


def pack_kernel(first, slots, elems, segs, subs, owners, targets, send_ref, at_ref, *scratch):
    owners_ref, targets_ref, seen, meta, sems = scratch
    copies = [
        pltpu.make_async_copy(owners, owners_ref, sems.at[0]),
        pltpu.make_async_copy(targets, targets_ref, sems.at[1]),
    ]
    for copy in copies:
        copy.start()
    rows, last = send_ref.shape[0], 3 * slots
    my_seg, my_sub = lax.axis_index("seg"), lax.axis_index("sub")
    lane = lax.broadcasted_iota(jnp.int32, (1, LANES), 1)
    meta[...] = jnp.zeros_like(meta)
    for r in range(rows):
        seen[r] = 0
    for copy in copies:
        copy.wait()

    def place(b, fullest):
        device, elem = divided(owners_ref[b], elems)
        device, sub = divided(device, subs)
        r, seg = divided(device, segs)
        apart = divided(seg - my_seg + segs, segs)[1]
        code = (apart + jnp.where(sub == my_sub, 0, segs)) * elems + elem
        k = seen[r]
        seen[r] = k + 1
        slot = k - first
        at_ref[b] = jnp.where(jnp.logical_and(slot >= 0, slot < slots), r * slots + slot, -1)

        @pl.when(jnp.logical_and(slot >= 0, slot < slots))
        def _():
            points = targets_ref[b]
            for a in range(3):
                send_ref[r, slot * 3 + a] = points[a : a + 1]
            added = jnp.where(lane == slot, code, jnp.where(lane == COUNT, 1, 0))
            meta[pl.ds(r, 1), :] += added

        return jnp.maximum(fullest, k + 1)

    fullest = lax.fori_loop(0, targets_ref.shape[0], place, jnp.int32(0), unroll=4)
    ids = jnp.where(lane == FULLEST, fullest, meta[...]).astype(jnp.float32)
    for r in range(rows):
        send_ref[r, last] = ids[r : r + 1]


def pack(owners, block_points, rows, first, slots, elems, segs, subs):
    blocks = owners.shape[0]
    return pl.pallas_call(
        functools.partial(pack_kernel, first, slots, elems, segs, subs),
        out_shape=[
            jax.ShapeDtypeStruct((rows, 3 * slots + 1, 1, LANES), jnp.float32),
            jax.ShapeDtypeStruct((blocks,), jnp.int32),
        ],
        in_specs=[pl.BlockSpec(memory_space=pltpu.HBM)] * 2,
        out_specs=[
            pl.BlockSpec(memory_space=pltpu.VMEM),
            pl.BlockSpec(memory_space=pltpu.SMEM),
        ],
        scratch_shapes=[
            pltpu.SMEM(owners.shape, jnp.int32),
            pltpu.VMEM(block_points.shape, jnp.float32),
            pltpu.SMEM((rows,), jnp.int32),
            pltpu.VMEM((rows, LANES), jnp.int32),
            pltpu.SemaphoreType.DMA((2,)),
        ],
        compiler_params=pltpu.CompilerParams(vmem_limit_bytes=4 << 20),
        name="pack",
    )(owners, block_points)


def newton(coef, target):
    def mapped(a, m):
        return coef[8 * a + m]

    def solve(jac, misfit):
        cof = [[None] * 3 for _ in range(3)]
        for r in range(3):
            r0, r1 = (r + 1) % 3, (r + 2) % 3
            for c in range(3):
                c0, c1 = (c + 1) % 3, (c + 2) % 3
                cof[r][c] = jac[r0][c0] * jac[r1][c1] - jac[r0][c1] * jac[r1][c0]
        det = jac[0][0] * cof[0][0] + jac[0][1] * cof[0][1] + jac[0][2] * cof[0][2]
        inverse = 1.0 / det
        return [
            (cof[0][c] * misfit[0] + cof[1][c] * misfit[1] + cof[2][c] * misfit[2]) * inverse
            for c in range(3)
        ]

    jac = [[mapped(a, 4), mapped(a, 2), mapped(a, 1)] for a in range(3)]
    step = solve(jac, [mapped(a, 0) - target[a] for a in range(3)])
    pos = [jnp.clip(-s, -1.2, 1.2) for s in step]
    for _ in range(NEWTON - 1):
        u, v, w = pos
        uv, uw, vw = u * v, u * w, v * w
        jac, misfit = [], []
        for a in range(3):
            du = mapped(a, 4) + mapped(a, 6) * v + mapped(a, 5) * w + mapped(a, 7) * vw
            dv = mapped(a, 2) + mapped(a, 6) * u + mapped(a, 3) * w + mapped(a, 7) * uw
            dw = mapped(a, 1) + mapped(a, 5) * u + mapped(a, 3) * v + mapped(a, 7) * uv
            at = mapped(a, 0) + mapped(a, 2) * v + mapped(a, 1) * w + mapped(a, 3) * vw + u * du
            jac.append([du, dv, dw])
            misfit.append(at - target[a])
        step = solve(jac, misfit)
        pos = [jnp.clip(p - s, -1.2, 1.2) for p, s in zip(pos, step)]
    return pos


def lagrange(point, table):
    value = (point - table[0]) * table[7]
    for k in range(1, 7):
        value = value * (point - table[k])
    return value


def halves(value):
    high = value.astype(jnp.bfloat16)
    return high, (value - high.astype(jnp.float32)).astype(jnp.bfloat16)


def segments(elems, lengths):
    size, found, piece, row = elems * 16, [], 0, 0
    for index, length in enumerate(lengths):
        here = 0
        while here < length:
            end = size if row < size else size + elems
            count = min(length - here, end - row)
            base = piece * size + row if row < size else piece * elems + row - size
            found.append((index, here, count, row >= size, base))
            here, row = here + count, row + count
            if row == size + elems:
                piece, row = piece + 1, 0
    return found


def evaluate_kernel(elems, slots, arrays, recv_ref, const_ref, *refs):
    pieces, (out_ref, fields, shapes, points, coefs, meta, live, sems) = refs[:arrays], refs[arrays:]
    senders = recv_ref.shape[0]
    ids = pltpu.make_async_copy(recv_ref.at[:, 3 * slots, 0, :], meta, sems.at[0])
    ids.start()
    copies = []
    for n, (index, row, count, of_coefs, there) in enumerate(
        segments(elems, [piece.shape[0] for piece in pieces])
    ):
        target = (shapes if of_coefs else fields).at[pl.ds(there, count)]
        source = pieces[index].at[pl.ds(row, count)]
        copies.append(pltpu.make_async_copy(source, target, sems.at[n + 1]))
    for copy in reversed(copies):
        copy.start()
    ids.wait()

    def of_sender(s, total):
        used = meta[s, COUNT].astype(jnp.int32)

        def of_slot(k, carry):
            live[total + k] = s * ID_LANES + k
            return carry

        lax.fori_loop(0, used, of_slot, 0)
        return total + used

    total = lax.fori_loop(0, senders, of_sender, jnp.int32(0))
    for copy in copies:
        copy.wait()

    lane = lax.broadcasted_iota(jnp.int32, (16, LANES), 1)
    upper = lax.broadcasted_iota(jnp.int32, (8, LANES), 0) < 4

    def gather(g):
        where = []
        for u in range(8):
            s, k = divided(live[jnp.clip(g * 8 + u, 0, jnp.maximum(total - 1, 0))], ID_LANES)
            code = meta[s, k].astype(jnp.int32)
            where += [s * slots + k, code * 16]
            for a in range(3):
                points[a, pl.ds(u, 1), :] = recv_ref[s, k * 3 + a]
            coefs[pl.ds(u, 1), :] = shapes[pl.ds(code, 1), :]
        all_coefs = coefs[...]
        coef = [jnp.broadcast_to(all_coefs[:, m : m + 1], (8, LANES)) for m in range(24)]
        return tuple(where) + tuple(newton(coef, [points[a] for a in range(3)]))

    def group(g, held):
        where, pos = held[:16], held[16:]
        following = gather(g + 1)
        for u in range(8):
            slot, start = where[2 * u : 2 * u + 2]
            along_x, along_y, along_z = [
                lagrange(jnp.broadcast_to(p[u : u + 1], (8, LANES)), const_ref) for p in pos
            ]
            weights = jnp.concatenate(
                [jnp.broadcast_to(along_y[j : j + 1], (8, LANES)) * along_z for j in range(8)], axis=0
            )
            weights = jnp.concatenate(halves(weights), axis=0)
            field = fields[pl.ds(pl.multiple_of(start, 16), 16), :]
            turned = pltpu.roll(field, LANES // 2, 1)
            even = jnp.where(lane < LANES // 2, field, turned)
            odd = jnp.where(lane < LANES // 2, turned, field)
            both = jnp.concatenate(halves(jnp.concatenate([even, odd], axis=0)), axis=0)
            sums = jnp.dot(both, weights, preferred_element_type=jnp.float32)
            total_x = None
            for q, i in enumerate((0, 4, 1, 5)):
                term = sums[8 * q : 8 * q + 8] + sums[32 + 8 * q : 40 + 8 * q]
                rows = [jnp.broadcast_to(along_x[r : r + 1], (8, LANES)) for r in (i, i + 2)]
                term = term * jnp.where(upper, rows[0], rows[1])
                total_x = term if total_x is None else total_x + term
            out_ref[slot] = total_x[0:4] + total_x[4:8]
        return following

    @pl.when(total > 0)
    def _():
        lax.fori_loop(0, (total + 7) // 8, group, gather(jnp.int32(0)))


def evaluate(recv, pieces, slots, elems):
    senders = recv.shape[0]
    return pl.pallas_call(
        functools.partial(evaluate_kernel, elems, slots, len(pieces)),
        out_shape=jax.ShapeDtypeStruct((senders * slots, 4, LANES), jnp.float32),
        in_specs=[pl.BlockSpec(memory_space=pltpu.VMEM)] * 2
        + [pl.BlockSpec(memory_space=pl.ANY)] * len(pieces),
        out_specs=pl.BlockSpec(memory_space=pltpu.VMEM),
        scratch_shapes=[
            pltpu.VMEM((8 * elems * 16, LANES), jnp.float32),
            pltpu.VMEM((8 * elems, LANES), jnp.float32),
            pltpu.VMEM((3, 8, LANES), jnp.float32),
            pltpu.VMEM((8, LANES), jnp.float32),
            pltpu.SMEM((senders, LANES), jnp.float32),
            pltpu.SMEM((senders * ID_LANES,), jnp.int32),
            pltpu.SemaphoreType.DMA((1 + len(segments(elems, [p.shape[0] for p in pieces])),)),
        ],
        compiler_params=pltpu.CompilerParams(vmem_limit_bytes=12 << 20),
        name="evaluate",
    )(recv, jnp.asarray(lagrange_constants()), *pieces)


def unpack_kernel(has_before, at_ref, back_ref, *refs):
    out_ref = refs[-1]
    for b in range(out_ref.shape[0]):
        if has_before:
            at = at_ref[b]
            taken = back_ref[jnp.maximum(at, 0)]
            out_ref[b] = jnp.where(at >= 0, taken, refs[0][b])
        else:
            out_ref[b] = back_ref[jnp.maximum(at_ref[b], 0)]


def unpack(at, back, before):
    held = [] if before is None else [before]
    return pl.pallas_call(
        functools.partial(unpack_kernel, before is not None),
        out_shape=jax.ShapeDtypeStruct((at.shape[0], 4, LANES), jnp.float32),
        in_specs=[pl.BlockSpec(memory_space=pltpu.SMEM)]
        + [pl.BlockSpec(memory_space=pltpu.VMEM)] * (1 + len(held)),
        out_specs=pl.BlockSpec(memory_space=pltpu.VMEM),
        compiler_params=pltpu.CompilerParams(vmem_limit_bytes=4 << 20),
        name="unpack",
    )(at, back, *held)


def row_pieces(old_fields, corner_shift):
    elems = old_fields.shape[0]
    table, offset = monomial_table()
    coefs = jnp.dot(jnp.asarray(table), corner_shift, precision=EXACT) + offset[:, None]
    coefs = jnp.pad(coefs.T, ((0, 0), (0, LANES - coefs.shape[0])))
    fields = old_fields.reshape(elems, 4, 4, LANES).transpose(0, 2, 1, 3).reshape(-1, LANES)
    own = jnp.concatenate([fields, coefs], axis=0)
    segs = lax.axis_size("seg")
    middle = own.shape[0] * 9 // 160 * 8

    def along(array, step):
        return lax.ppermute(array, "seg", [(i, (i + step) % segs) for i in range(segs)])

    def swapped(array):
        return lax.ppermute(array, "sub", [(0, 1), (1, 0)])

    before = along(own, 1)
    after = along(own, segs - 1)
    near = along(own[:middle], 2)
    far = along(before[middle:], 1)
    opposite = [jnp.concatenate([near, far], axis=0)]
    swaps = [swapped(own), swapped(after)]
    swaps += [swapped(opposite[0]), swapped(before)]
    return [own, after, *opposite, before, *swaps]


def all_to_all(array):
    return lax.all_to_all(array, "block", split_axis=0, concat_axis=0, tiled=True)


def shards(old_fields, corner_shift, targets, owners):
    rows = lax.axis_size("block")
    segs, subs = lax.axis_size("seg"), lax.axis_size("sub")
    elems = old_fields.shape[0]
    most = CAP * segs * subs
    block_points = targets.reshape(3, owners.shape[0], -1).transpose(1, 0, 2)
    pieces = row_pieces(old_fields, corner_shift)

    def trip(first, slots, before):
        send, at = pack(owners, block_points, rows, first, slots, elems, segs, subs)
        recv = all_to_all(send)
        answers = evaluate(recv, pieces, slots, elems).reshape(rows, slots, 4, LANES)
        back = all_to_all(answers).reshape(rows * slots, 4, LANES)
        return unpack(at, back, before), recv[:, 3 * slots, 0, FULLEST]

    done, fullest = trip(0, FIRST, None)
    done = lax.cond(
        jnp.max(fullest) > FIRST,
        lambda held: trip(FIRST, most - FIRST, held)[0],
        lambda held: held,
        done,
    )
    return done.transpose(1, 0, 2).reshape(4, -1)


def solution(mesh):
    split = ("groups", "block", "seg", "sub")
    in_specs = (P(split, None, None), P(None, split), P(None, split), P(split))
    return jax.shard_map(
        shards, mesh=mesh, in_specs=in_specs, out_specs=P(None, split), check_vma=False
    )
```
